512 devices in a mesh: aper: 64 (over z_lo, y, x), rng: 4 (over z_hi), beam: 2 (over core).
Axes of the slice: x: 4, y: 4, z: 16 (z_hi: 4, z_lo: 4; z = z_hi * 4 + z_lo), core: 2. Of those that a mesh axis runs over, the one named last changes fastest.
Arguments:
- children: float32 [64, 2, 8192, 256], P('aper', None, 'rng', 'beam'), may hold values from -6 to 6
- shift_one: int32 [2, 256], replicated, may hold values from -8 to 8
- rtaps_one: float32 [2, 8, 256], replicated, may hold values from -2 to 2
- bstart_one: int32 [2, 512], replicated, may hold values from -5 to 252, as said below
- btaps_one: float32 [2, 8, 512], replicated, may hold values from -2 to 2
- prate_one: float32 [2, 512], replicated, may hold values from -64 to 64
- poff_one: float32 [2, 512], replicated, may hold values from -3.140625 to 3.140625
- shift_two: int32 [2, 512], replicated, may hold values from -8 to 8
- rtaps_two: float32 [2, 8, 512], replicated, may hold values from -2 to 2
- bstart_two: int32 [2, 1024], replicated, may hold values from -5 to 508, as said below
- btaps_two: float32 [2, 8, 1024], replicated, may hold values from -2 to 2
- prate_two: float32 [2, 1024], replicated, may hold values from -64 to 64
- poff_two: float32 [2, 1024], replicated, may hold values from -3.140625 to 3.140625
Outputs:
- merged: float32 [64, 2, 8192, 256], P('aper', None, 'rng', 'beam')
The draws below stay inside these ranges and needn't reach their ends.
Inputs may be any that keep to these rules, and one draw needn't show every extreme that they name: bstart_one[c, b] is b // 2 - 8 // 2 plus -1, 0 or 1. bstart_two[c, b] is b // 2 - 8 // 2 plus -1, 0 or 1.
All inputs are finite; a program needn't handle non-finite values.
Results may differ from the reference program's by a relative error of at most 0.0003.
Values sent between devices are 32-bit elements; how exact they have to be, the bound alone decides.
A program may use at most 64 MiB of HBM per device.

```python
import jax
import jax.numpy as jnp
from jax import lax

BEAMS = 256
RTAPS = 8
BTAPS = 8
SHIFT = 8
RRIM = 12
RANGE = 8192
SUBAPS = 64
N_BEAM = 2


def draw_bstart_one(key, part):
    base_rows = jnp.arange(2 * BEAMS, dtype=jnp.int32) // 2 - BTAPS // 2
    jitter = jax.random.randint(jax.random.fold_in(key, 11), (2, 2 * BEAMS), -1, 2)
    return (base_rows[None, :] + jitter).astype(jnp.int32)


def draw_bstart_two(key, part):
    base_rows = jnp.arange(4 * BEAMS, dtype=jnp.int32) // 2 - BTAPS // 2
    jitter = jax.random.randint(jax.random.fold_in(key, 23), (2, 4 * BEAMS), -1, 2)
    return (base_rows[None, :] + jitter).astype(jnp.int32)


def with_ends(drawn, rng, least, largest):
    longest = drawn.shape.index(max(drawn.shape))
    spots = []
    for shift in (0, 1):
        where = [jax.random.randint(jax.random.fold_in(rng, axis), (), 0, length) for axis, length in enumerate(drawn.shape)]
        where[longest] = (where[longest] + shift) % drawn.shape[longest]
        spots.append(tuple(where))
    return drawn.at[spots[0]].set(least).at[spots[1]].set(largest)


def block_scale(key, extent, shards, least, high):
    def one(position, shards_of):
        heights = jax.random.uniform(jax.random.fold_in(jax.random.fold_in(key, 6), position), (shards_of,), jnp.float32, least / len(shards), high / len(shards))
        return jnp.repeat(jnp.exp(heights), extent[position] // shards_of).reshape((-1,) + (1,) * (len(extent) - position - 1))

    loudness = one(*shards[0])
    for cut in shards[1:]:
        loudness = loudness * one(*cut)
    return loudness


def bell_draw(key, shape, scale, most, split=(), held_as=jnp.bfloat16):
    drawn = jax.random.normal(key, shape, jnp.float32) * scale
    if len(split) > 0:
        drawn = block_scale(key, shape, split, -0.22, 0.18) * drawn
    return jnp.clip(drawn, min=-most, max=most).astype(held_as)


def setup_inputs(seed: int = 0) -> dict:
    seeds = jax.random.split(jax.random.key(seed), 14)
    return {
        "children": bell_draw(seeds[0], (SUBAPS, 2, RANGE, BEAMS), 1.0, 6.0, ((0, 64), (2, 4), (3, 2)), jnp.float32),
        "shift_one": with_ends(jax.random.randint(seeds[1], (2, BEAMS), -SHIFT, SHIFT + 1), jax.random.fold_in(seeds[1], 1), -SHIFT, SHIFT).astype(jnp.int32),
        "rtaps_one": bell_draw(seeds[2], (2, RTAPS, BEAMS), RTAPS ** -0.5, 2.0, (), jnp.float32),
        "bstart_one": draw_bstart_one(jax.random.fold_in(seeds[13], 71), 0),
        "btaps_one": bell_draw(seeds[4], (2, BTAPS, 2 * BEAMS), BTAPS ** -0.5, 2.0, (), jnp.float32),
        "prate_one": jnp.clip(jax.random.uniform(seeds[5], (2, 2 * BEAMS), jnp.float32, -64.0, 64.0), -64.0, 64.0),
        "poff_one": jnp.clip(jax.random.uniform(seeds[6], (2, 2 * BEAMS), jnp.float32, -3.140625, 3.140625), -3.140625, 3.140625),
        "shift_two": with_ends(jax.random.randint(seeds[7], (2, 2 * BEAMS), -SHIFT, SHIFT + 1), jax.random.fold_in(seeds[7], 1), -SHIFT, SHIFT).astype(jnp.int32),
        "rtaps_two": bell_draw(seeds[8], (2, RTAPS, 2 * BEAMS), RTAPS ** -0.5, 2.0, (), jnp.float32),
        "bstart_two": draw_bstart_two(jax.random.fold_in(seeds[13], 71), 0),
        "btaps_two": bell_draw(seeds[10], (2, BTAPS, 4 * BEAMS), BTAPS ** -0.5, 2.0, (), jnp.float32),
        "prate_two": jnp.clip(jax.random.uniform(seeds[11], (2, 4 * BEAMS), jnp.float32, -64.0, 64.0), -64.0, 64.0),
        "poff_two": jnp.clip(jax.random.uniform(seeds[12], (2, 4 * BEAMS), jnp.float32, -3.140625, 3.140625), -3.140625, 3.140625),
    }


def range_interp(child_image, shifts, weights):
    rows_all = child_image.shape[1]
    padded = jnp.pad(child_image, ((0, 0), (RRIM, RRIM), (0, 0)))
    base_rows = jnp.arange(rows_all, dtype=jnp.int32)[:, None] + RRIM + shifts.astype(jnp.int32)[None, :]
    summed = jnp.zeros(child_image.shape, jnp.float32)
    for tap_index in range(RTAPS):
        row_index = jnp.broadcast_to((base_rows + (tap_index - RTAPS // 2)).astype(jnp.int32)[None], child_image.shape)
        summed = summed + weights[tap_index][None, None, :] * jnp.take_along_axis(padded, row_index, axis=1)
    return summed


def beam_interp(level_vals, starts, weights, rates, offsets, range_frac):
    ext_width = level_vals.shape[2]
    col_count = starts.shape[0]
    column_ids = lax.broadcasted_iota(jnp.int32, (ext_width, col_count, BTAPS), 0)
    taps_at = starts.astype(jnp.int32)[None, :, None] + lax.broadcasted_iota(jnp.int32, (ext_width, col_count, BTAPS), 2)
    matrix = jnp.sum(jnp.where(column_ids == taps_at, jnp.transpose(weights)[None], jnp.zeros((), jnp.float32)), axis=2)
    rows_all = level_vals.shape[1]
    mixed_vals = jnp.dot(level_vals.reshape(2 * rows_all, ext_width), matrix, precision=lax.Precision.HIGHEST, preferred_element_type=jnp.float32).reshape(2, rows_all, col_count)
    phase_angle = range_frac[:, None] * rates[None, :] + offsets[None, :]
    cosine = jnp.cos(phase_angle)
    sine_part = jnp.sin(phase_angle)
    return jnp.stack([cosine * mixed_vals[0] - sine_part * mixed_vals[1], sine_part * mixed_vals[0] + cosine * mixed_vals[1]])


def merge_ref(left_image, right_image, tables, range_frac):
    shift_tab, rtap_tab, start_tab, btap_tab, rate_tab, off_tab = tables
    summed = None
    for side_index, child_image in ((0, left_image), (1, right_image)):
        level_vals = range_interp(child_image, shift_tab[side_index], rtap_tab[side_index])
        term = beam_interp(level_vals, start_tab[side_index], btap_tab[side_index], rate_tab[side_index], off_tab[side_index], range_frac)
        summed = term if summed is None else summed + term
    return summed


def reference(children, shift_one, rtaps_one, bstart_one, btaps_one, prate_one, poff_one, shift_two, rtaps_two, bstart_two, btaps_two, prate_two, poff_two):
    rows_all = children.shape[2]
    range_frac = jnp.arange(rows_all, dtype=jnp.int32).astype(jnp.float32) / rows_all
    tables_one = (shift_one, rtaps_one, bstart_one, btaps_one, prate_one, poff_one)
    tables_two = (shift_two, rtaps_two, bstart_two, btaps_two, prate_two, poff_two)
    group_count = children.shape[0] // 4
    groups = children.reshape(group_count, 4, 2, rows_all, BEAMS)

    def one_group(quartet):
        left_parent = merge_ref(quartet[0], quartet[2], tables_one, range_frac)
        right_parent = merge_ref(quartet[1], quartet[3], tables_one, range_frac)
        return merge_ref(left_parent, right_parent, tables_two, range_frac)

    finals = lax.map(one_group, groups)
    beam_block = BEAMS // N_BEAM
    shaped = finals.reshape(group_count, 2, rows_all, N_BEAM, 4, beam_block)
    shaped = jnp.transpose(shaped, (0, 4, 1, 2, 3, 5))
    return shaped.reshape(group_count * 4, 2, rows_all, BEAMS)
```

```python
import functools

import jax
import jax.numpy as jnp
from jax import lax
from jax.experimental import pallas as pl
from jax.experimental.pallas import tpu as pltpu
from jax.sharding import PartitionSpec as P

MESH = pl.DeviceIdType.MESH
ROWS = 2048
BEAM = 128
CHUNK = 256
CHUNKS = ROWS // CHUNK
FIRST = 5
WIN = 48
TAPS = 8
OFFS = 24
RIM = 16
TOP = 32
SUB = 16
F32 = jnp.float32
BF16 = jnp.bfloat16


def split_bf16(x):
    hi = x.astype(BF16)
    lo = (x - hi.astype(F32)).astype(BF16)
    return hi, lo


def range_table(shift_row, tap_rows, out_ref):
    for o in range(OFFS):
        acc = jnp.zeros((1, BEAM), F32)
        for k in range(TAPS):
            acc = acc + jnp.where(shift_row + (8 + k) == o, tap_rows[k : k + 1], 0.0)
        out_ref[o] = jnp.broadcast_to(acc, (8, BEAM))


def beam_matrix(rows, start_row, tap_rows):
    ids = lax.broadcasted_iota(jnp.int32, (rows, BEAM), 0)
    acc = jnp.zeros((rows, BEAM), F32)
    for k in range(TAPS):
        acc = acc + jnp.where(ids == start_row + k, tap_rows[k : k + 1], 0.0)
    return acc


def phase_tables(rate, off, base, lead, near_c, near_s, far_c, far_s, tmp_c, tmp_s):
    scale = 1.0 / 8192.0
    r8 = lax.broadcasted_iota(jnp.int32, (8, BEAM), 0).astype(F32) * scale
    r32 = (lax.broadcasted_iota(jnp.int32, (32, BEAM), 0) * 8).astype(F32) * scale
    r16 = (base + lax.broadcasted_iota(jnp.int32, (16, BEAM), 0) * CHUNK - lead).astype(F32) * scale
    far = rate * r16 + off
    far_c[...] = jnp.cos(far)
    far_s[...] = jnp.sin(far)
    small = rate * r8
    sc, ss = jnp.cos(small), jnp.sin(small)
    big = rate * r32
    tmp_c[...] = jnp.cos(big)
    tmp_s[...] = jnp.sin(big)

    def fill(q, carry):
        bc = tmp_c[pl.ds(q, 1), :]
        bs = tmp_s[pl.ds(q, 1), :]
        at = pl.ds(pl.multiple_of(q * 8, 8), 8)
        near_c[at, :] = bc * sc - bs * ss
        near_s[at, :] = bs * sc + bc * ss
        return carry

    lax.fori_loop(0, 32, fill, 0)


def kernel(
    child_hbm,
    sh1,
    rt1,
    bs1,
    bt1,
    pr1,
    po1,
    sh2,
    rt2,
    bs2,
    bt2,
    pr2,
    po2,
    out,
    child,
    wide,
    turned,
    got,
    mixed,
    parent,
    packed,
    tab1,
    tab2,
    mat1,
    mat2a,
    mat2b,
    near_c,
    near_s,
    far_c,
    far_s,
    tmp_c,
    tmp_s,
    in_sem,
    zs_sem,
    zr_sem,
    ps_sem,
    pr_sem,
    es_sem,
    er_sem,
    xs_sem,
    xr_sem,
):
    aper = lax.axis_index("aper")
    rng = lax.axis_index("rng")
    beam = lax.axis_index("beam")
    me = lax.rem(aper, 4)
    group = aper - me
    block = 4 * beam + me
    up, down = lax.rem(rng + 3, 4), lax.rem(rng + 1, 4)

    def peer(d):
        return lax.rem(me + d, 4)

    def chunk_of(t):
        return lax.rem(t + FIRST, CHUNKS)

    load = pltpu.make_async_copy(child_hbm.at[0], child.at[:, pl.ds(RIM, ROWS), :], in_sem)
    load.start()

    barrier = pltpu.get_barrier_semaphore()
    for d in (1, 2, 3):
        pl.semaphore_signal(
            barrier, inc=1, device_id=(group + peer(d), rng, beam), device_id_type=MESH
        )
    pl.semaphore_signal(barrier, inc=1, device_id=(aper, rng, 1 - beam), device_id_type=MESH)
    pl.semaphore_signal(barrier, inc=1, device_id=(aper, up, beam), device_id_type=MESH)
    pl.semaphore_signal(barrier, inc=1, device_id=(aper, down, beam), device_id_type=MESH)

    @pl.when(beam == 0)
    def _():
        turned[:, 0:8, :] = jnp.zeros((2, 8, ROWS), F32)

    @pl.when(beam == 1)
    def _():
        turned[:, 136:144, :] = jnp.zeros((2, 8, ROWS), F32)

    side = lax.div(me, 2)
    own = pl.ds(pl.multiple_of(beam * BEAM, BEAM), BEAM)
    shift_row = jnp.where(side == 0, sh1[0:1, own], sh1[1:2, own])
    range_table(shift_row, rt1[side, :, own], tab1)

    pl.semaphore_wait(barrier, 6)
    load.wait()

    def halo(buf, sem_s, sem_r, first, last, low, high):
        return (
            pltpu.make_async_remote_copy(
                src_ref=buf.at[:, pl.ds(first, RIM), :],
                dst_ref=buf.at[:, pl.ds(high, RIM), :],
                send_sem=sem_s.at[0],
                recv_sem=sem_r.at[0],
                device_id=(aper, up, beam),
                device_id_type=MESH,
            ),
            pltpu.make_async_remote_copy(
                src_ref=buf.at[:, pl.ds(last, RIM), :],
                dst_ref=buf.at[:, pl.ds(low, RIM), :],
                send_sem=sem_s.at[1],
                recv_sem=sem_r.at[1],
                device_id=(aper, down, beam),
                device_id_type=MESH,
            ),
        )

    zc = halo(child, zs_sem, zr_sem, RIM, ROWS, 0, RIM + ROWS)
    zp = halo(parent, ps_sem, pr_sem, TOP, TOP + ROWS - RIM, TOP - RIM, TOP + ROWS)
    for c in zc:
        c.start()

    def edge_copy(t):
        at = pl.ds(pl.multiple_of(chunk_of(t) * CHUNK, CHUNK), CHUNK)
        return pltpu.make_async_remote_copy(
            src_ref=turned.at[:, pl.ds(pl.multiple_of(128 - 120 * beam, 8), 8), at],
            dst_ref=turned.at[:, pl.ds(pl.multiple_of(136 * beam, 8), 8), at],
            send_sem=es_sem.at[t],
            recv_sem=er_sem.at[t],
            device_id=(aper, rng, 1 - beam),
            device_id_type=MESH,
        )

    def window_copy(t, d):
        at = pl.ds(pl.multiple_of(chunk_of(t) * CHUNK, CHUNK), CHUNK)
        to = peer(d)
        return pltpu.make_async_remote_copy(
            src_ref=turned.at[:, pl.ds(pl.multiple_of(32 * to, 8), WIN), at],
            dst_ref=got.at[me, :, :, at],
            send_sem=xs_sem.at[d - 1, t],
            recv_sem=xr_sem.at[d - 1, t],
            device_id=(group + to, rng, beam),
            device_id_type=MESH,
        )

    def produce(t):
        j = chunk_of(t)
        base = pl.multiple_of(j * CHUNK, CHUNK)

        def rows(s, carry):
            first = base + s * 32
            for comp in range(2):
                acc = [jnp.zeros((8, BEAM), F32) for _ in range(4)]
                for o in range(OFFS):
                    w = tab1[o]
                    for v in range(4):
                        acc[v] = acc[v] + w * child[comp, pl.ds(first + (o + 4 + 8 * v), 8), :]
                for v in range(4):
                    wide[comp, pl.ds(pl.multiple_of(s * 32 + 8 * v, 8), 8), :] = acc[v]
            return carry

        lax.fori_loop(0, CHUNK // 32, rows, 0)
        for comp in range(2):
            for half in range(CHUNK // BEAM):
                turned[
                    comp, 8:136, pl.ds(pl.multiple_of(base + half * BEAM, BEAM), BEAM)
                ] = jnp.transpose(wide[comp, half * BEAM : (half + 1) * BEAM, :])

    def send(t):
        edge_copy(t).wait_recv()
        for d in (1, 3, 2):
            window_copy(t, d).start()
        at = pl.ds(pl.multiple_of(chunk_of(t) * CHUNK, CHUNK), CHUNK)
        got[me, :, :, at] = turned[:, pl.ds(pl.multiple_of(32 * me, 8), WIN), at]

    def produce_step(t, carry):
        @pl.when(t == 2)
        def _():
            for c in zc:
                c.wait_recv()

            @pl.when(rng == 0)
            def _():
                child[:, 0:RIM, :] = jnp.zeros((2, RIM, BEAM), F32)

            @pl.when(rng == 3)
            def _():
                child[:, RIM + ROWS :, :] = jnp.zeros((2, RIM, BEAM), F32)

        produce(t)
        edge_copy(t).start()

        @pl.when(t > 0)
        def _():
            send(t - 1)

        return carry

    lax.fori_loop(0, CHUNKS, produce_step, 0)
    send(CHUNKS - 1)

    shift = lax.rem(520 - 64 * block, 512)

    def lanes(v):
        return pltpu.roll(v, shift, 1)[:, :BEAM]

    ints = lanes(jnp.concatenate([bs1[...], sh2[...], bs1[...], sh2[...]], axis=0))
    floats = lanes(jnp.concatenate([pr1[...], po1[...], pr1[...], po1[...]], axis=0))
    beams_here = lax.broadcasted_iota(jnp.int32, (TAPS, BEAM), 1) + (64 * block - 8)
    inside = jnp.logical_and(beams_here >= 0, beams_here < 512)
    final = pl.ds(pl.multiple_of(block * BEAM, BEAM), BEAM)
    for s in range(2):
        taps = jnp.where(inside, lanes(bt1[s]), 0.0)
        m = beam_matrix(WIN, ints[s : s + 1] - (32 * block - 8), taps)
        hi, lo = split_bf16(m)
        mat1[s, 0:WIN, :] = hi
        mat1[s, WIN : 2 * WIN, :] = hi
        mat1[s, 2 * WIN : 3 * WIN, :] = lo
        range_table(ints[2 + s : 3 + s], lanes(rt2[s]), tab2.at[s])
        m = beam_matrix(BEAM, bs2[s : s + 1, final] - (64 * block - 8), bt2[s, :, final])
        hi, lo = split_bf16(m)
        mat2a[s, 0:BEAM, :] = hi
        mat2a[s, BEAM : 2 * BEAM, :] = hi
        mat2b[s] = lo
        phase_tables(
            floats[s : s + 1],
            floats[2 + s : 3 + s],
            rng * ROWS,
            0,
            near_c.at[s],
            near_s.at[s],
            far_c.at[s],
            far_s.at[s],
            tmp_c,
            tmp_s,
        )
        phase_tables(
            pr2[s : s + 1, final],
            po2[s : s + 1, final],
            rng * ROWS,
            RIM,
            near_c.at[2 + s],
            near_s.at[2 + s],
            far_c.at[2 + s],
            far_s.at[2 + s],
            tmp_c,
            tmp_s,
        )

    def turn(level, j, rho):
        both = []
        for s in range(2):
            fc = far_c[2 * level + s, pl.ds(j, 1), :]
            fs = far_s[2 * level + s, pl.ds(j, 1), :]
            nc = near_c[2 * level + s, pl.ds(rho, SUB), :]
            ns = near_s[2 * level + s, pl.ds(rho, SUB), :]
            both.append((fc * nc - fs * ns, fs * nc + fc * ns))
        return both

    def make_parents(j):
        at = pl.ds(pl.multiple_of(j * CHUNK, CHUNK), CHUNK)
        for c in range(4):
            for comp in range(2):
                hi, lo = split_bf16(got[c, comp, :, at])
                mixed[2 * c + comp] = lax.dot_general(
                    jnp.concatenate([hi, lo, hi], axis=0),
                    mat1[c // 2],
                    (((0,), (0,)), ((), ())),
                    preferred_element_type=F32,
                )

        def rows(s, carry):
            rho = pl.multiple_of(s * SUB, SUB)
            (c0, s0), (c1, s1) = turn(0, j, rho)
            here = pl.ds(rho, SUB)
            to = pl.ds(pl.multiple_of(TOP + j * CHUNK + rho, SUB), SUB)
            for e in range(2):
                lr, li = mixed[2 * e, here, :], mixed[2 * e + 1, here, :]
                rr, ri = mixed[4 + 2 * e, here, :], mixed[5 + 2 * e, here, :]
                parent[2 * e, to, :] = (c0 * lr - s0 * li) + (c1 * rr - s1 * ri)
                parent[2 * e + 1, to, :] = (s0 * lr + c0 * li) + (s1 * rr + c1 * ri)
            return carry

        lax.fori_loop(0, CHUNK // SUB, rows, 0)

    def range_two(first, slot):
        for e in range(2):
            acc = [[jnp.zeros((8, BEAM), F32) for _ in range(2)] for _ in range(2)]
            for o in range(OFFS):
                w = tab2[e, o]
                for comp in range(2):
                    for v in range(2):
                        acc[comp][v] = acc[comp][v] + w * parent[
                            2 * e + comp, pl.ds(first + (TOP - 12 + o + 8 * v), 8), :
                        ]
            for comp in range(2):
                hi, lo = split_bf16(jnp.concatenate(acc[comp], axis=0))
                packed[2 * e + comp, pl.ds(slot, SUB), 0:BEAM] = hi
                packed[2 * e + comp, pl.ds(slot, SUB), BEAM : 2 * BEAM] = lo

    def products(count):
        for e in range(2):
            for comp in range(2):
                z = packed[2 * e + comp, 0:count, :]
                mixed[2 * e + comp, 0:count, :] = jnp.dot(
                    z, mat2a[e], preferred_element_type=F32
                ) + jnp.dot(z[:, :BEAM], mat2b[e], preferred_element_type=F32)

    def finish(first, slot, j, rho):
        (c0, s0), (c1, s1) = turn(1, j, rho)
        here = pl.ds(slot, SUB)
        to = pl.ds(first, SUB)
        lr, li, rr, ri = (mixed[i, here, :] for i in range(4))
        out[0, 0, to, :] = (c0 * lr - s0 * li) + (c1 * rr - s1 * ri)
        out[0, 1, to, :] = (s0 * lr + c0 * li) + (s1 * rr + c1 * ri)

    def consume_step(t, carry):
        j = chunk_of(t)
        for d in (1, 3, 2):
            window_copy(t, d).wait_recv()
        make_parents(j)

        @pl.when(j == 0)
        def _():
            for c in zp:
                c.start()

        begin = jnp.where(jnp.logical_or(t == 0, j == 0), 2, 0)

        def rows_in(s, carry):
            slot = pl.multiple_of(s * SUB, SUB)
            range_two(pl.multiple_of(j * CHUNK - RIM + slot, SUB), slot)
            return carry

        def rows_out(s, carry):
            slot = pl.multiple_of(s * SUB, SUB)
            finish(pl.multiple_of(j * CHUNK - RIM + slot, SUB), slot, j, slot)
            return carry

        lax.fori_loop(begin, CHUNK // SUB, rows_in, 0)
        products(CHUNK)
        lax.fori_loop(begin, CHUNK // SUB, rows_out, 0)
        return carry

    lax.fori_loop(0, CHUNKS, consume_step, 0)

    for c in zp:
        c.wait_recv()

    @pl.when(rng == 0)
    def _():
        parent[:, TOP - RIM : TOP, :] = jnp.zeros((4, RIM, BEAM), F32)

    @pl.when(rng == 3)
    def _():
        parent[:, TOP + ROWS : TOP + ROWS + RIM, :] = jnp.zeros((4, RIM, BEAM), F32)

    joint = FIRST * CHUNK
    strips = (
        (0, 0, RIM),
        (joint - RIM, FIRST, 0),
        (joint, FIRST, RIM),
        (ROWS - RIM, CHUNKS, 0),
    )
    for n, (first, j, rho) in enumerate(strips):
        range_two(first, n * SUB)
    products(len(strips) * SUB)
    for n, (first, j, rho) in enumerate(strips):
        finish(first, n * SUB, j, rho)

    for c in zc + zp:
        c.wait_send()

    def drain(t, carry):
        edge_copy(t).wait_send()
        for d in (1, 3, 2):
            window_copy(t, d).wait_send()
        return carry

    lax.fori_loop(0, CHUNKS, drain, 0)


def body(*args):
    vmem = pl.BlockSpec(memory_space=pltpu.VMEM)
    dma = pltpu.SemaphoreType.DMA
    return pl.pallas_call(
        kernel,
        out_shape=jax.ShapeDtypeStruct((1, 2, ROWS, BEAM), F32),
        in_specs=[pl.BlockSpec(memory_space=pl.ANY)] + [vmem] * 12,
        out_specs=vmem,
        scratch_shapes=[
            pltpu.VMEM((2, ROWS + 2 * RIM, BEAM), F32),
            pltpu.VMEM((2, CHUNK, BEAM), F32),
            pltpu.VMEM((2, BEAM + 16, ROWS), F32),
            pltpu.VMEM((4, 2, WIN, ROWS), F32),
            pltpu.VMEM((8, CHUNK, BEAM), F32),
            pltpu.VMEM((4, TOP + ROWS + 32, BEAM), F32),
            pltpu.VMEM((4, CHUNK, 2 * BEAM), BF16),
            pltpu.VMEM((OFFS, 8, BEAM), F32),
            pltpu.VMEM((2, OFFS, 8, BEAM), F32),
            pltpu.VMEM((2, 3 * WIN, BEAM), BF16),
            pltpu.VMEM((2, 2 * BEAM, BEAM), BF16),
            pltpu.VMEM((2, BEAM, BEAM), BF16),
            pltpu.VMEM((4, CHUNK, BEAM), F32),
            pltpu.VMEM((4, CHUNK, BEAM), F32),
            pltpu.VMEM((4, 16, BEAM), F32),
            pltpu.VMEM((4, 16, BEAM), F32),
            pltpu.VMEM((32, BEAM), F32),
            pltpu.VMEM((32, BEAM), F32),
            dma,
            dma((2,)),
            dma((2,)),
            dma((2,)),
            dma((2,)),
            dma((CHUNKS,)),
            dma((CHUNKS,)),
            dma((3, CHUNKS)),
            dma((3, CHUNKS)),
        ],
        compiler_params=pltpu.CompilerParams(
            collective_id=0, has_side_effects=True, vmem_limit_bytes=40 * 2**20
        ),
        name="merge",
    )(*args)


def solution(mesh):
    return jax.shard_map(
        body,
        mesh=mesh,
        in_specs=(P("aper", None, "rng", "beam"),) + (P(),) * 12,
        out_specs=P("aper", None, "rng", "beam"),
        check_vma=False,
    )
```

```python
import functools

import jax
import jax.numpy as jnp
from jax import lax
from jax.experimental import pallas as pl
from jax.experimental.pallas import tpu as pltpu
from jax.sharding import PartitionSpec as P

MESH = pl.DeviceIdType.MESH
ROWS = 2048
BEAM = 128
CHUNK = 128
CHUNKS = ROWS // CHUNK
FIRST = 7
EARLY = 3
LEAD = 6
NEAR = CHUNK + 32
FAR = 24
WIN = 48
TAPS = 8
OFFS = 24
RIM = 16
TOP = 32
SUB = 16
F32 = jnp.float32
BF16 = jnp.bfloat16


def split_bf16(x):
    hi = x.astype(BF16)
    lo = (x - hi.astype(F32)).astype(BF16)
    return hi, lo


def range_table(shift_row, tap_rows, out_ref):
    for o in range(OFFS):
        acc = jnp.zeros((1, BEAM), F32)
        for k in range(TAPS):
            acc = acc + jnp.where(shift_row + (8 + k) == o, tap_rows[k : k + 1], 0.0)
        out_ref[o] = jnp.broadcast_to(acc, (8, BEAM))


def beam_matrix(rows, start_row, tap_rows):
    ids = lax.broadcasted_iota(jnp.int32, (rows, BEAM), 0)
    acc = jnp.zeros((rows, BEAM), F32)
    for k in range(TAPS):
        acc = acc + jnp.where(ids == start_row + k, tap_rows[k : k + 1], 0.0)
    return acc


def phase_tables(rate, off, base, lead, near_c, near_s, far_c, far_s, tmp_c, tmp_s):
    scale = 1.0 / 8192.0
    r8 = lax.broadcasted_iota(jnp.int32, (8, BEAM), 0).astype(F32) * scale
    r24 = (lax.broadcasted_iota(jnp.int32, (24, BEAM), 0) * 8).astype(F32) * scale
    rows = base + lax.broadcasted_iota(jnp.int32, (FAR, BEAM), 0) * CHUNK - lead
    far = rate * (rows.astype(F32) * scale) + off
    far_c[...] = jnp.cos(far)
    far_s[...] = jnp.sin(far)
    small = rate * r8
    sc, ss = jnp.cos(small), jnp.sin(small)
    big = rate * r24
    tmp_c[...] = jnp.cos(big)
    tmp_s[...] = jnp.sin(big)

    def fill(q, carry):
        bc = tmp_c[pl.ds(q, 1), :]
        bs = tmp_s[pl.ds(q, 1), :]
        at = pl.ds(pl.multiple_of(q * 8, 8), 8)
        near_c[at, :] = bc * sc - bs * ss
        near_s[at, :] = bs * sc + bc * ss
        return carry

    lax.fori_loop(0, NEAR // 8, fill, 0)


def kernel(
    child_hbm,
    sh1_hbm,
    rt1_hbm,
    bs1_hbm,
    bt1_hbm,
    pr1_hbm,
    po1_hbm,
    sh2_hbm,
    rt2_hbm,
    bs2_hbm,
    bt2_hbm,
    pr2_hbm,
    po2_hbm,
    out,
    sh1,
    rt1,
    bs1,
    bt1,
    pr1,
    po1,
    sh2,
    rt2,
    bs2,
    bt2,
    pr2,
    po2,
    child,
    wide,
    turned,
    got,
    mixed,
    parent,
    packed,
    image,
    tab1,
    tab2,
    mat1,
    mat2a,
    mat2b,
    near_c,
    near_s,
    far_c,
    far_s,
    tmp_c,
    tmp_s,
    in_sem,
    out_sem,
    tab_sem,
    chip_sem,
    core_sem,
    zs_sem,
    zr_sem,
    ps_sem,
    pr_sem,
    es_sem,
    er_sem,
    xs_sem,
    xr_sem,
):
    aper = lax.axis_index("aper")
    rng = lax.axis_index("rng")
    beam = lax.axis_index("beam")
    me = lax.rem(aper, 4)
    group = aper - me
    block = 4 * beam + me
    up, down = lax.rem(rng + 3, 4), lax.rem(rng + 1, 4)

    def peer(d):
        return lax.rem(me + d, 4)

    def chunk_of(t):
        return lax.rem(t + FIRST, CHUNKS)

    load = pltpu.make_async_copy(child_hbm.at[0], child.at[:, pl.ds(RIM, ROWS), :], in_sem)
    tables = [
        pltpu.make_async_copy(src, dst, tab_sem.at[n])
        for n, (src, dst) in enumerate(
            (
                (sh1_hbm, sh1),
                (rt1_hbm, rt1),
                (bs1_hbm, bs1),
                (bt1_hbm, bt1),
                (pr1_hbm, pr1),
                (po1_hbm, po1),
                (sh2_hbm, sh2),
                (rt2_hbm, rt2),
                (bs2_hbm, bs2),
                (bt2_hbm, bt2),
                (pr2_hbm, pr2),
                (po2_hbm, po2),
            )
        )
    ]
    for c in tables[:2]:
        c.start()
    load.start()
    for c in tables[2:]:
        c.start()

    barrier = pltpu.get_barrier_semaphore()
    partner = (aper, rng, 1 - beam)

    @pl.when(beam == 0)
    def _():
        for d in (1, 2, 3):
            pl.semaphore_signal(
                barrier, inc=1, device_id=(group + peer(d), rng, beam), device_id_type=MESH
            )

    @pl.when(beam == 1)
    def _():
        pl.semaphore_signal(barrier, inc=1, device_id=partner, device_id_type=MESH)

    @pl.when(beam == 0)
    def _():
        turned[:, 0:8, :] = jnp.zeros((2, 8, ROWS), F32)

    @pl.when(beam == 1)
    def _():
        turned[:, 136:144, :] = jnp.zeros((2, 8, ROWS), F32)

    for c in tables[:2]:
        c.wait()
    side = lax.div(me, 2)
    own = pl.ds(pl.multiple_of(beam * BEAM, BEAM), BEAM)
    shift_row = jnp.where(side == 0, sh1[0:1, own], sh1[1:2, own])
    range_table(shift_row, rt1[side, :, own], tab1)

    def halo(buf, sem_s, sem_r, first, last, low, high):
        return (
            pltpu.make_async_remote_copy(
                src_ref=buf.at[:, pl.ds(first, RIM), :],
                dst_ref=buf.at[:, pl.ds(high, RIM), :],
                send_sem=sem_s.at[0],
                recv_sem=sem_r.at[0],
                device_id=(aper, up, beam),
                device_id_type=MESH,
            ),
            pltpu.make_async_remote_copy(
                src_ref=buf.at[:, pl.ds(last, RIM), :],
                dst_ref=buf.at[:, pl.ds(low, RIM), :],
                send_sem=sem_s.at[1],
                recv_sem=sem_r.at[1],
                device_id=(aper, down, beam),
                device_id_type=MESH,
            ),
        )

    zc = halo(child, zs_sem, zr_sem, RIM, ROWS, 0, RIM + ROWS)
    zp = halo(parent, ps_sem, pr_sem, TOP, TOP + ROWS - RIM, TOP - RIM, TOP + ROWS)

    def edge_copy(t):
        at = pl.ds(pl.multiple_of(chunk_of(t) * CHUNK, CHUNK), CHUNK)
        return pltpu.make_async_remote_copy(
            src_ref=turned.at[:, pl.ds(pl.multiple_of(128 - 120 * beam, 8), 8), at],
            dst_ref=turned.at[:, pl.ds(pl.multiple_of(136 * beam, 8), 8), at],
            send_sem=es_sem.at[t],
            recv_sem=er_sem.at[t],
            device_id=(aper, rng, 1 - beam),
            device_id_type=MESH,
        )

    def window_copy(t, d):
        at = pl.ds(pl.multiple_of(chunk_of(t) * CHUNK, CHUNK), CHUNK)
        to = peer(d)
        return pltpu.make_async_remote_copy(
            src_ref=turned.at[:, pl.ds(pl.multiple_of(32 * to, 8), WIN), at],
            dst_ref=got.at[me, :, :, at],
            send_sem=xs_sem.at[d - 1, t],
            recv_sem=xr_sem.at[d - 1, t],
            device_id=(group + to, rng, beam),
            device_id_type=MESH,
        )

    def produce(t):
        j = chunk_of(t)
        base = pl.multiple_of(j * CHUNK, CHUNK)

        def rows(s, carry):
            first = base + s * 32
            for comp in range(2):
                acc = [jnp.zeros((8, BEAM), F32) for _ in range(4)]
                for o in range(OFFS):
                    w = tab1[o]
                    for v in range(4):
                        acc[v] = acc[v] + w * child[comp, pl.ds(first + (o + 4 + 8 * v), 8), :]
                for v in range(4):
                    wide[comp, pl.ds(pl.multiple_of(s * 32 + 8 * v, 8), 8), :] = acc[v]
            return carry

        lax.fori_loop(0, CHUNK // 32, rows, 0)
        for comp in range(2):
            for half in range(CHUNK // BEAM):
                turned[
                    comp, 8:136, pl.ds(pl.multiple_of(base + half * BEAM, BEAM), BEAM)
                ] = jnp.transpose(wide[comp, half * BEAM : (half + 1) * BEAM, :])

    def send(t):
        edge_copy(t).wait_recv()
        for d in (1, 3, 2):
            window_copy(t, d).start()
        at = pl.ds(pl.multiple_of(chunk_of(t) * CHUNK, CHUNK), CHUNK)
        got[me, :, :, at] = turned[:, pl.ds(pl.multiple_of(32 * me, 8), WIN), at]

    load.wait()
    for t in range(EARLY):
        produce(t)

    @pl.when(beam == 0)
    def _():
        pl.semaphore_wait(barrier, 4)
        for d in (1, 2, 3):
            pl.semaphore_signal(
                chip_sem, inc=1, device_id=(group + peer(d), rng, beam), device_id_type=MESH
            )
        pl.semaphore_wait(chip_sem, 3)
        pl.semaphore_signal(core_sem, inc=1, device_id=partner, device_id_type=MESH)

    @pl.when(beam == 1)
    def _():
        pl.semaphore_wait(core_sem, 1)
        for z in (up, down):
            pl.semaphore_signal(barrier, inc=1, device_id=(aper, z, beam), device_id_type=MESH)

    for t in range(EARLY):
        edge_copy(t).start()
    for t in range(EARLY, LEAD):
        produce(t)
        edge_copy(t).start()
        if t == EARLY:
            for before in range(EARLY):
                send(before)
        else:
            send(t - 1)

    for c in tables[2:]:
        c.wait()
    shift = lax.rem(520 - 64 * block, 512)

    def lanes(v):
        return pltpu.roll(v, shift, 1)[:, :BEAM]

    ints = lanes(jnp.concatenate([bs1[...], sh2[...], bs1[...], sh2[...]], axis=0))
    floats = lanes(jnp.concatenate([pr1[...], po1[...], pr1[...], po1[...]], axis=0))
    beams_here = lax.broadcasted_iota(jnp.int32, (TAPS, BEAM), 1) + (64 * block - 8)
    inside = jnp.logical_and(beams_here >= 0, beams_here < 512)
    final = pl.ds(pl.multiple_of(block * BEAM, BEAM), BEAM)
    for s in range(2):
        taps = jnp.where(inside, lanes(bt1[s]), 0.0)
        m = beam_matrix(WIN, ints[s : s + 1] - (32 * block - 8), taps)
        hi, lo = split_bf16(m)
        mat1[s, 0:WIN, :] = hi
        mat1[s, WIN : 2 * WIN, :] = hi
        mat1[s, 2 * WIN : 3 * WIN, :] = lo
        range_table(ints[2 + s : 3 + s], lanes(rt2[s]), tab2.at[s])
        m = beam_matrix(BEAM, bs2[s : s + 1, final] - (64 * block - 8), bt2[s, :, final])
        hi, lo = split_bf16(m)
        mat2a[s, 0:BEAM, :] = hi
        mat2a[s, BEAM : 2 * BEAM, :] = hi
        mat2b[s] = lo
        phase_tables(
            floats[s : s + 1],
            floats[2 + s : 3 + s],
            rng * ROWS,
            0,
            near_c.at[s],
            near_s.at[s],
            far_c.at[s],
            far_s.at[s],
            tmp_c,
            tmp_s,
        )
        phase_tables(
            pr2[s : s + 1, final],
            po2[s : s + 1, final],
            rng * ROWS,
            RIM,
            near_c.at[2 + s],
            near_s.at[2 + s],
            far_c.at[2 + s],
            far_s.at[2 + s],
            tmp_c,
            tmp_s,
        )

    @pl.when(beam == 1)
    def _():
        pl.semaphore_wait(barrier, 2)
        pl.semaphore_signal(core_sem, inc=1, device_id=partner, device_id_type=MESH)

    @pl.when(beam == 0)
    def _():
        pl.semaphore_wait(core_sem, 1)

    for c in zc:
        c.start()

    def turn(level, j, rho):
        both = []
        for s in range(2):
            fc = far_c[2 * level + s, pl.ds(j, 1), :]
            fs = far_s[2 * level + s, pl.ds(j, 1), :]
            nc = near_c[2 * level + s, pl.ds(rho, SUB), :]
            ns = near_s[2 * level + s, pl.ds(rho, SUB), :]
            both.append((fc * nc - fs * ns, fs * nc + fc * ns))
        return both

    def make_parents(j):
        at = pl.ds(pl.multiple_of(j * CHUNK, CHUNK), CHUNK)
        for c in range(4):
            for comp in range(2):
                hi, lo = split_bf16(got[c, comp, :, at])
                mixed[2 * c + comp, 0:CHUNK, :] = lax.dot_general(
                    jnp.concatenate([hi, lo, hi], axis=0),
                    mat1[c // 2],
                    (((0,), (0,)), ((), ())),
                    preferred_element_type=F32,
                )

        def rows(s, carry):
            rho = pl.multiple_of(s * SUB, SUB)
            (c0, s0), (c1, s1) = turn(0, j, rho)
            here = pl.ds(rho, SUB)
            to = pl.ds(pl.multiple_of(TOP + j * CHUNK + rho, SUB), SUB)
            for e in range(2):
                lr, li = mixed[2 * e, here, :], mixed[2 * e + 1, here, :]
                rr, ri = mixed[4 + 2 * e, here, :], mixed[5 + 2 * e, here, :]
                parent[2 * e, to, :] = (c0 * lr - s0 * li) + (c1 * rr - s1 * ri)
                parent[2 * e + 1, to, :] = (s0 * lr + c0 * li) + (s1 * rr + c1 * ri)
            return carry

        lax.fori_loop(0, CHUNK // SUB, rows, 0)

    def range_two(first, slot, e, weights):
        acc = [[jnp.zeros((8, BEAM), F32) for _ in range(2)] for _ in range(2)]
        for o in range(OFFS):
            for comp in range(2):
                for v in range(2):
                    acc[comp][v] = acc[comp][v] + weights[o] * parent[
                        2 * e + comp, pl.ds(first + (TOP - 12 + o + 8 * v), 8), :
                    ]
        for comp in range(2):
            hi, lo = split_bf16(jnp.concatenate(acc[comp], axis=0))
            packed[2 * e + comp, pl.ds(slot, SUB), 0:BEAM] = hi
            packed[2 * e + comp, pl.ds(slot, SUB), BEAM : 2 * BEAM] = lo

    def range_weights(e):
        return [tab2[e, o] for o in range(OFFS)]

    def products(count):
        for e in range(2):
            for comp in range(2):
                z = packed[2 * e + comp, 0:count, :]
                mixed[2 * e + comp, 0:count, :] = jnp.dot(
                    z, mat2a[e], preferred_element_type=F32
                ) + jnp.dot(z[:, :BEAM], mat2b[e], preferred_element_type=F32)

    def finish(first, slot, j, rho):
        (c0, s0), (c1, s1) = turn(1, j, rho)
        here = pl.ds(slot, SUB)
        to = pl.ds(first, SUB)
        lr, li, rr, ri = (mixed[i, here, :] for i in range(4))
        image[0, to, :] = (c0 * lr - s0 * li) + (c1 * rr - s1 * ri)
        image[1, to, :] = (s0 * lr + c0 * li) + (s1 * rr + c1 * ri)

    def put(j):
        at = pl.ds(pl.multiple_of(j * CHUNK, CHUNK), CHUNK)
        return pltpu.make_async_copy(image.at[:, at, :], out.at[0, :, at, :], out_sem.at[j])

    def consume(t, begin, end):
        j = chunk_of(t)
        for d in (1, 3, 2):
            window_copy(t, d).wait_recv()
        make_parents(j)

        def rows_in(s, carry, e, weights):
            slot = pl.multiple_of(s * SUB, SUB)
            range_two(pl.multiple_of(j * CHUNK - RIM + slot, SUB), slot, e, weights)
            return carry

        def rows_out(s, carry):
            slot = pl.multiple_of(s * SUB, SUB)
            finish(pl.multiple_of(j * CHUNK - RIM + slot, SUB), slot, j, slot)
            return carry

        for e in range(2):
            lax.fori_loop(
                begin, end, functools.partial(rows_in, e=e, weights=range_weights(e)), 0
            )
        products(end * SUB)
        lax.fori_loop(begin, end, rows_out, 0)

    def step(t, carry):
        j = chunk_of(t)

        @pl.when(t + LEAD - 1 < CHUNKS)
        def _():
            send(t + LEAD - 1)

        @pl.when(t + LEAD < CHUNKS)
        def _():
            @pl.when(t + LEAD == CHUNKS - 1 - FIRST)
            def _():
                for c in zc:
                    c.wait_recv()

                @pl.when(rng == 0)
                def _():
                    child[:, 0:RIM, :] = jnp.zeros((2, RIM, BEAM), F32)

                @pl.when(rng == 3)
                def _():
                    child[:, RIM + ROWS :, :] = jnp.zeros((2, RIM, BEAM), F32)

            produce(t + LEAD)
            edge_copy(t + LEAD).start()

        consume(t, jnp.where(jnp.logical_or(t == 0, j == 0), 2, 0), CHUNK // SUB)

        @pl.when(j == 0)
        def _():
            zp[0].start()

        @pl.when(j == CHUNKS - 1)
        def _():
            zp[1].start()

        whole = jnp.logical_and(t > 1, jnp.logical_and(j != 0, j != 1))

        @pl.when(whole)
        def _():
            put(j - 1).start()

        return carry

    lax.fori_loop(0, CHUNKS - 1, step, 0)

    consume(CHUNKS - 1, 0, CHUNK // SUB + 2)
    put(FIRST - 2).start()
    put(FIRST - 1).start()
    put(FIRST).start()

    for c in zp:
        c.wait_recv()

    @pl.when(rng == 0)
    def _():
        parent[:, TOP - RIM : TOP, :] = jnp.zeros((4, RIM, BEAM), F32)

    @pl.when(rng == 3)
    def _():
        parent[:, TOP + ROWS : TOP + ROWS + RIM, :] = jnp.zeros((4, RIM, BEAM), F32)

    ends = ((0, 0, RIM), (ROWS - RIM, CHUNKS, 0))
    for n, (first, j, rho) in enumerate(ends):
        for e in range(2):
            range_two(first, n * SUB, e, range_weights(e))
    products(len(ends) * SUB)
    for n, (first, j, rho) in enumerate(ends):
        finish(first, n * SUB, j, rho)
    put(0).start()
    put(CHUNKS - 1).start()

    for c in zc + zp:
        c.wait_send()

    def drain(t, carry):
        put(t).wait()
        edge_copy(t).wait_send()
        for d in (1, 3, 2):
            window_copy(t, d).wait_send()
        return carry

    lax.fori_loop(0, CHUNKS, drain, 0)


def body(*args):
    dma = pltpu.SemaphoreType.DMA
    return pl.pallas_call(
        kernel,
        out_shape=jax.ShapeDtypeStruct((1, 2, ROWS, BEAM), F32),
        in_specs=[pl.BlockSpec(memory_space=pl.ANY)] * 13,
        out_specs=pl.BlockSpec(memory_space=pl.ANY),
        scratch_shapes=[pltpu.VMEM(a.shape, a.dtype) for a in args[1:]]
        + [
            pltpu.VMEM((2, ROWS + 2 * RIM, BEAM), F32),
            pltpu.VMEM((2, CHUNK, BEAM), F32),
            pltpu.VMEM((2, BEAM + 16, ROWS), F32),
            pltpu.VMEM((4, 2, WIN, ROWS), F32),
            pltpu.VMEM((8, NEAR, BEAM), F32),
            pltpu.VMEM((4, TOP + ROWS + 32, BEAM), F32),
            pltpu.VMEM((4, NEAR, 2 * BEAM), BF16),
            pltpu.VMEM((2, ROWS, BEAM), F32),
            pltpu.VMEM((OFFS, 8, BEAM), F32),
            pltpu.VMEM((2, OFFS, 8, BEAM), F32),
            pltpu.VMEM((2, 3 * WIN, BEAM), BF16),
            pltpu.VMEM((2, 2 * BEAM, BEAM), BF16),
            pltpu.VMEM((2, BEAM, BEAM), BF16),
            pltpu.VMEM((4, NEAR, BEAM), F32),
            pltpu.VMEM((4, NEAR, BEAM), F32),
            pltpu.VMEM((4, FAR, BEAM), F32),
            pltpu.VMEM((4, FAR, BEAM), F32),
            pltpu.VMEM((24, BEAM), F32),
            pltpu.VMEM((24, BEAM), F32),
            dma,
            dma((CHUNKS,)),
            dma((12,)),
            pltpu.SemaphoreType.REGULAR,
            pltpu.SemaphoreType.REGULAR,
            dma((2,)),
            dma((2,)),
            dma((2,)),
            dma((2,)),
            dma((CHUNKS,)),
            dma((CHUNKS,)),
            dma((3, CHUNKS)),
            dma((3, CHUNKS)),
        ],
        compiler_params=pltpu.CompilerParams(
            collective_id=0, has_side_effects=True, vmem_limit_bytes=60 * 2**20
        ),
        name="merge",
    )(*args)


def solution(mesh):
    return jax.shard_map(
        body,
        mesh=mesh,
        in_specs=(P("aper", None, "rng", "beam"),) + (P(),) * 12,
        out_specs=P("aper", None, "rng", "beam"),
        check_vma=False,
    )
```

```python
import functools

import jax
import jax.numpy as jnp
from jax import lax
from jax.experimental import pallas as pl
from jax.experimental.pallas import tpu as pltpu
from jax.sharding import PartitionSpec as P

MESH = pl.DeviceIdType.MESH
ROWS = 2048
BEAM = 128
CHUNK = 128
CHUNKS = ROWS // CHUNK
FIRST = 7
EARLY = 1
LEAD = 6
NEAR = CHUNK + 32
FAR = 24
WIN = 48
TAPS = 8
FINE = 12
COARSE = 4
RIM = 16
TOP = 32
SUB = 16
F32 = jnp.float32
BF16 = jnp.bfloat16


def split_bf16(x):
    hi = x.astype(BF16)
    lo = (x - hi.astype(F32)).astype(BF16)
    return hi, lo


def range_table(shift_row, tap_rows, out_ref, step_ref):
    shift = shift_row + 8
    q = jnp.minimum(lax.shift_right_logical(shift, 2), COARSE - 1)
    p = shift - 4 * q
    step_ref[...] = jnp.broadcast_to(q, (8, BEAM))
    for o in range(FINE):
        acc = jnp.zeros((1, BEAM), F32)
        for k in range(TAPS):
            acc = acc + jnp.where(p + k == o, tap_rows[k : k + 1], 0.0)
        out_ref[o] = jnp.broadcast_to(acc, (8, BEAM))


def fine_rows(src, comps, first, weights, dst, slot):
    for n, comp in enumerate(comps):
        for v in range(2):
            acc = None
            for o in range(FINE):
                term = weights[o] * src[comp, pl.ds(first + (o + 8 * v), 8), :]
                acc = term if acc is None else acc + term
            dst[n, pl.ds(pl.multiple_of(slot + 8 * v, 8), 8), :] = acc


def coarse_rows(src, comp, slot, picks):
    out = []
    for v in range(2):
        rows = [src[comp, pl.ds(slot + (4 * q + 8 * v), 8), :] for q in range(COARSE)]
        low = jnp.where(picks[0], rows[0], rows[1])
        high = jnp.where(picks[2], rows[2], rows[3])
        out.append(jnp.where(picks[1], low, high))
    return out


def picks_of(step_ref):
    q = step_ref[...]
    return [q == 0, q < 2, q == 2]


def beam_matrix(rows, start_row, tap_rows):
    ids = lax.broadcasted_iota(jnp.int32, (rows, BEAM), 0)
    acc = jnp.zeros((rows, BEAM), F32)
    for k in range(TAPS):
        acc = acc + jnp.where(ids == start_row + k, tap_rows[k : k + 1], 0.0)
    return acc


def phase_tables(rate, off, base, lead, near_c, near_s, far_c, far_s, tmp_c, tmp_s):
    scale = 1.0 / 8192.0
    r8 = lax.broadcasted_iota(jnp.int32, (8, BEAM), 0).astype(F32) * scale
    r24 = (lax.broadcasted_iota(jnp.int32, (24, BEAM), 0) * 8).astype(F32) * scale
    rows = base + lax.broadcasted_iota(jnp.int32, (FAR, BEAM), 0) * CHUNK - lead
    far = rate * (rows.astype(F32) * scale) + off
    far_c[...] = jnp.cos(far)
    far_s[...] = jnp.sin(far)
    small = rate * r8
    sc, ss = jnp.cos(small), jnp.sin(small)
    big = rate * r24
    tmp_c[...] = jnp.cos(big)
    tmp_s[...] = jnp.sin(big)

    def fill(q, carry):
        bc = tmp_c[pl.ds(q, 1), :]
        bs = tmp_s[pl.ds(q, 1), :]
        at = pl.ds(pl.multiple_of(q * 8, 8), 8)
        near_c[at, :] = bc * sc - bs * ss
        near_s[at, :] = bs * sc + bc * ss
        return carry

    lax.fori_loop(0, NEAR // 8, fill, 0)


def kernel(
    child_hbm,
    sh1_hbm,
    rt1_hbm,
    bs1_hbm,
    bt1_hbm,
    pr1_hbm,
    po1_hbm,
    sh2_hbm,
    rt2_hbm,
    bs2_hbm,
    bt2_hbm,
    pr2_hbm,
    po2_hbm,
    out,
    sh1,
    rt1,
    bs1,
    bt1,
    pr1,
    po1,
    sh2,
    rt2,
    bs2,
    bt2,
    pr2,
    po2,
    child,
    wide,
    turned,
    got,
    mixed,
    parent,
    packed,
    image,
    tab1,
    tab2,
    step1,
    step2,
    fine,
    mat1,
    mat2a,
    mat2b,
    near_c,
    near_s,
    far_c,
    far_s,
    tmp_c,
    tmp_s,
    in_sem,
    out_sem,
    tab_sem,
    chip_sem,
    core_sem,
    zs_sem,
    zr_sem,
    ps_sem,
    pr_sem,
    es_sem,
    er_sem,
    xs_sem,
    xr_sem,
):
    aper = lax.axis_index("aper")
    rng = lax.axis_index("rng")
    beam = lax.axis_index("beam")
    me = lax.rem(aper, 4)
    group = aper - me
    block = 4 * beam + me
    up, down = lax.rem(rng + 3, 4), lax.rem(rng + 1, 4)

    def peer(d):
        return lax.rem(me + d, 4)

    def chunk_of(t):
        return lax.rem(t + FIRST, CHUNKS)

    cut = (0, FIRST * CHUNK - RIM, (FIRST + EARLY) * CHUNK + RIM, ROWS)
    loads = [
        pltpu.make_async_copy(
            child_hbm.at[0, :, pl.ds(cut[n], cut[n + 1] - cut[n]), :],
            child.at[:, pl.ds(RIM + cut[n], cut[n + 1] - cut[n]), :],
            in_sem.at[n],
        )
        for n in (1, 2, 0)
    ]
    tables = [
        pltpu.make_async_copy(src, dst, tab_sem.at[n])
        for n, (src, dst) in enumerate(
            (
                (sh1_hbm, sh1),
                (rt1_hbm, rt1),
                (bs1_hbm, bs1),
                (bt1_hbm, bt1),
                (pr1_hbm, pr1),
                (po1_hbm, po1),
                (sh2_hbm, sh2),
                (rt2_hbm, rt2),
                (bs2_hbm, bs2),
                (bt2_hbm, bt2),
                (pr2_hbm, pr2),
                (po2_hbm, po2),
            )
        )
    ]
    for c in tables[:2]:
        c.start()
    for c in loads:
        c.start()
    for c in tables[2:]:
        c.start()

    barrier = pltpu.get_barrier_semaphore()
    partner = (aper, rng, 1 - beam)

    @pl.when(beam == 0)
    def _():
        for d in (1, 2, 3):
            pl.semaphore_signal(
                barrier, inc=1, device_id=(group + peer(d), rng, beam), device_id_type=MESH
            )

    @pl.when(beam == 1)
    def _():
        pl.semaphore_signal(barrier, inc=1, device_id=partner, device_id_type=MESH)

    @pl.when(beam == 0)
    def _():
        pl.semaphore_wait(barrier, 4)
        for d in (1, 2, 3):
            pl.semaphore_signal(
                chip_sem, inc=1, device_id=(group + peer(d), rng, beam), device_id_type=MESH
            )

    @pl.when(beam == 0)
    def _():
        turned[:, 0:8, :] = jnp.zeros((2, 8, ROWS), F32)

    @pl.when(beam == 1)
    def _():
        turned[:, 136:144, :] = jnp.zeros((2, 8, ROWS), F32)

    for c in tables[:2]:
        c.wait()
    side = lax.div(me, 2)
    own = pl.ds(pl.multiple_of(beam * BEAM, BEAM), BEAM)
    shift_row = jnp.where(side == 0, sh1[0:1, own], sh1[1:2, own])
    range_table(shift_row, rt1[side, :, own], tab1, step1)

    def halo(buf, sem_s, sem_r, first, last, low, high):
        return (
            pltpu.make_async_remote_copy(
                src_ref=buf.at[:, pl.ds(first, RIM), :],
                dst_ref=buf.at[:, pl.ds(high, RIM), :],
                send_sem=sem_s.at[0],
                recv_sem=sem_r.at[0],
                device_id=(aper, up, beam),
                device_id_type=MESH,
            ),
            pltpu.make_async_remote_copy(
                src_ref=buf.at[:, pl.ds(last, RIM), :],
                dst_ref=buf.at[:, pl.ds(low, RIM), :],
                send_sem=sem_s.at[1],
                recv_sem=sem_r.at[1],
                device_id=(aper, down, beam),
                device_id_type=MESH,
            ),
        )

    zc = halo(child, zs_sem, zr_sem, RIM, ROWS, 0, RIM + ROWS)
    zp = halo(parent, ps_sem, pr_sem, TOP, TOP + ROWS - RIM, TOP - RIM, TOP + ROWS)

    def edge_copy(t):
        at = pl.ds(pl.multiple_of(chunk_of(t) * CHUNK, CHUNK), CHUNK)
        return pltpu.make_async_remote_copy(
            src_ref=turned.at[:, pl.ds(pl.multiple_of(128 - 120 * beam, 8), 8), at],
            dst_ref=turned.at[:, pl.ds(pl.multiple_of(136 * beam, 8), 8), at],
            send_sem=es_sem.at[t],
            recv_sem=er_sem.at[t],
            device_id=(aper, rng, 1 - beam),
            device_id_type=MESH,
        )

    def window_copy(t, d):
        at = pl.ds(pl.multiple_of(chunk_of(t) * CHUNK, CHUNK), CHUNK)
        to = peer(d)
        return pltpu.make_async_remote_copy(
            src_ref=turned.at[:, pl.ds(pl.multiple_of(32 * to, 8), WIN), at],
            dst_ref=got.at[me, :, :, at],
            send_sem=xs_sem.at[d - 1, t],
            recv_sem=xr_sem.at[d - 1, t],
            device_id=(group + to, rng, beam),
            device_id_type=MESH,
        )

    def produce(t):
        j = chunk_of(t)
        base = pl.multiple_of(j * CHUNK, CHUNK)

        weights = [tab1[o] for o in range(FINE)]
        picks = picks_of(step1)

        def fine_in(s, carry):
            slot = pl.multiple_of(s * SUB, SUB)
            fine_rows(child, (0, 1), base + (RIM - 16) + slot, weights, fine, slot)
            return carry

        def coarse_in(s, carry):
            slot = pl.multiple_of(s * SUB, SUB)
            for comp in range(2):
                for v, x in enumerate(coarse_rows(fine, comp, slot + 4, picks)):
                    wide[comp, pl.ds(pl.multiple_of(slot + 8 * v, 8), 8), :] = x
            return carry

        lax.fori_loop(0, CHUNK // SUB + 1, fine_in, 0)
        lax.fori_loop(0, CHUNK // SUB, coarse_in, 0)
        for comp in range(2):
            for half in range(CHUNK // BEAM):
                turned[
                    comp, 8:136, pl.ds(pl.multiple_of(base + half * BEAM, BEAM), BEAM)
                ] = jnp.transpose(wide[comp, half * BEAM : (half + 1) * BEAM, :])

    def inner(d):
        return jnp.logical_or(peer(d) == 1, peer(d) == 2)

    def send(t):
        edge_copy(t).wait_recv()
        for d in (1, 3, 2):
            window_copy(t, d).start()
        keep(t)

    def keep(t):
        at = pl.ds(pl.multiple_of(chunk_of(t) * CHUNK, CHUNK), CHUNK)
        got[me, :, :, at] = turned[:, pl.ds(pl.multiple_of(32 * me, 8), WIN), at]

    loads[0].wait()
    produce(0)

    def open_windows():
        edge_copy(0).start()
        for d in (1, 3, 2):

            @pl.when(inner(d))
            def _(d=d):
                window_copy(0, d).start()

    @pl.when(beam == 0)
    def _():
        open_windows()
        pl.semaphore_wait(chip_sem, 3)
        pl.semaphore_signal(core_sem, inc=1, device_id=partner, device_id_type=MESH)

    @pl.when(beam == 1)
    def _():
        pl.semaphore_wait(core_sem, 1)
        for z in (up, down):
            pl.semaphore_signal(barrier, inc=1, device_id=(aper, z, beam), device_id_type=MESH)
        open_windows()

    loads[1].wait()
    produce(1)
    edge_copy(1).start()
    edge_copy(0).wait_recv()
    for d in (1, 3, 2):

        @pl.when(jnp.logical_not(inner(d)))
        def _(d=d):
            window_copy(0, d).start()

    keep(0)
    loads[2].wait()

    def lead_step(t, carry):
        produce(t)
        edge_copy(t).start()
        send(t - 1)
        return carry

    lax.fori_loop(2, LEAD, lead_step, 0)

    @pl.when(beam == 1)
    def _():
        pl.semaphore_wait(barrier, 2)
        pl.semaphore_signal(core_sem, inc=1, device_id=partner, device_id_type=MESH)

    @pl.when(beam == 0)
    def _():
        pl.semaphore_wait(core_sem, 1)

    for c in zc:
        c.start()

    for c in tables[2:]:
        c.wait()
    shift = lax.rem(520 - 64 * block, 512)

    def lanes(v):
        return pltpu.roll(v, shift, 1)[:, :BEAM]

    ints = lanes(jnp.concatenate([bs1[...], sh2[...], bs1[...], sh2[...]], axis=0))
    floats = lanes(jnp.concatenate([pr1[...], po1[...], pr1[...], po1[...]], axis=0))
    beams_here = lax.broadcasted_iota(jnp.int32, (TAPS, BEAM), 1) + (64 * block - 8)
    inside = jnp.logical_and(beams_here >= 0, beams_here < 512)
    final = pl.ds(pl.multiple_of(block * BEAM, BEAM), BEAM)
    for s in range(2):
        taps = jnp.where(inside, lanes(bt1[s]), 0.0)
        m = beam_matrix(WIN, ints[s : s + 1] - (32 * block - 8), taps)
        hi, lo = split_bf16(m)
        mat1[s, 0:WIN, :] = hi
        mat1[s, WIN : 2 * WIN, :] = hi
        mat1[s, 2 * WIN : 3 * WIN, :] = lo
        range_table(ints[2 + s : 3 + s], lanes(rt2[s]), tab2.at[s], step2.at[s])
        m = beam_matrix(BEAM, bs2[s : s + 1, final] - (64 * block - 8), bt2[s, :, final])
        hi, lo = split_bf16(m)
        mat2a[s, 0:BEAM, :] = hi
        mat2a[s, BEAM : 2 * BEAM, :] = hi
        mat2b[s] = lo
        phase_tables(
            floats[s : s + 1],
            floats[2 + s : 3 + s],
            rng * ROWS,
            0,
            near_c.at[s],
            near_s.at[s],
            far_c.at[s],
            far_s.at[s],
            tmp_c,
            tmp_s,
        )
        phase_tables(
            pr2[s : s + 1, final],
            po2[s : s + 1, final],
            rng * ROWS,
            RIM,
            near_c.at[2 + s],
            near_s.at[2 + s],
            far_c.at[2 + s],
            far_s.at[2 + s],
            tmp_c,
            tmp_s,
        )

    def turn(level, j, rho):
        both = []
        for s in range(2):
            fc = far_c[2 * level + s, pl.ds(j, 1), :]
            fs = far_s[2 * level + s, pl.ds(j, 1), :]
            nc = near_c[2 * level + s, pl.ds(rho, SUB), :]
            ns = near_s[2 * level + s, pl.ds(rho, SUB), :]
            both.append((fc * nc - fs * ns, fs * nc + fc * ns))
        return both

    def make_parents(j):
        at = pl.ds(pl.multiple_of(j * CHUNK, CHUNK), CHUNK)
        for c in range(4):
            both = jnp.concatenate([got[c, 0, :, at], got[c, 1, :, at]], axis=1)
            hi, lo = split_bf16(both)
            mixed[2 * c : 2 * c + 2, 0:CHUNK, :] = lax.dot_general(
                jnp.concatenate([hi, lo, hi], axis=0),
                mat1[c // 2],
                (((0,), (0,)), ((), ())),
                preferred_element_type=F32,
            ).reshape(2, CHUNK, BEAM)

        def rows(s, carry):
            rho = pl.multiple_of(s * SUB, SUB)
            (c0, s0), (c1, s1) = turn(0, j, rho)
            here = pl.ds(rho, SUB)
            to = pl.ds(pl.multiple_of(TOP + j * CHUNK + rho, SUB), SUB)
            for e in range(2):
                lr, li = mixed[2 * e, here, :], mixed[2 * e + 1, here, :]
                rr, ri = mixed[4 + 2 * e, here, :], mixed[5 + 2 * e, here, :]
                parent[2 * e, to, :] = (c0 * lr - s0 * li) + (c1 * rr - s1 * ri)
                parent[2 * e + 1, to, :] = (s0 * lr + c0 * li) + (s1 * rr + c1 * ri)
            return carry

        lax.fori_loop(0, CHUNK // SUB, rows, 0)

    def fine_two(first, slot, e, weights):
        fine_rows(
            parent, (2 * e, 2 * e + 1), first + TOP, weights, fine.at[pl.ds(2 * e, 2)], slot
        )

    def coarse_two(slot, from_slot, e, picks):
        for comp in range(2):
            rows = coarse_rows(fine, 2 * e + comp, from_slot + 4, picks)
            hi, lo = split_bf16(jnp.concatenate(rows, axis=0))
            packed[2 * e + comp, pl.ds(slot, SUB), 0:BEAM] = hi
            packed[2 * e + comp, pl.ds(slot, SUB), BEAM : 2 * BEAM] = lo

    def weights_two(e):
        return [tab2[e, o] for o in range(FINE)]

    def products(count):
        for e in range(2):
            z = packed[2 * e : 2 * e + 2, 0:count, :].reshape(2 * count, 2 * BEAM)
            mixed[2 * e : 2 * e + 2, 0:count, :] = (
                jnp.dot(z, mat2a[e], preferred_element_type=F32)
                + jnp.dot(z[:, :BEAM], mat2b[e], preferred_element_type=F32)
            ).reshape(2, count, BEAM)

    def finish(first, slot, j, rho):
        (c0, s0), (c1, s1) = turn(1, j, rho)
        here = pl.ds(slot, SUB)
        to = pl.ds(first, SUB)
        lr, li, rr, ri = (mixed[i, here, :] for i in range(4))
        image[0, to, :] = (c0 * lr - s0 * li) + (c1 * rr - s1 * ri)
        image[1, to, :] = (s0 * lr + c0 * li) + (s1 * rr + c1 * ri)

    def put(j):
        at = pl.ds(pl.multiple_of(j * CHUNK, CHUNK), CHUNK)
        return pltpu.make_async_copy(image.at[:, at, :], out.at[0, :, at, :], out_sem.at[j])

    def consume(t, begin, end):
        j = chunk_of(t)
        for d in (1, 3, 2):
            window_copy(t, d).wait_recv()
        make_parents(j)

        def fine_in(s, carry, e, weights):
            slot = pl.multiple_of(s * SUB, SUB)
            fine_two(j * CHUNK - 2 * RIM + slot, slot, e, weights)
            return carry

        def coarse_in(s, carry, e, picks):
            slot = pl.multiple_of(s * SUB, SUB)
            coarse_two(slot, slot, e, picks)
            return carry

        def rows_out(s, carry):
            slot = pl.multiple_of(s * SUB, SUB)
            finish(pl.multiple_of(j * CHUNK - RIM + slot, SUB), slot, j, slot)
            return carry

        for e in range(2):
            lax.fori_loop(
                begin, end + 1, functools.partial(fine_in, e=e, weights=weights_two(e)), 0
            )
            lax.fori_loop(
                begin, end, functools.partial(coarse_in, e=e, picks=picks_of(step2.at[e])), 0
            )
        products(end * SUB)
        lax.fori_loop(begin, end, rows_out, 0)

    def step(t, carry):
        j = chunk_of(t)

        @pl.when(t + LEAD - 1 < CHUNKS)
        def _():
            send(t + LEAD - 1)

        @pl.when(t + LEAD < CHUNKS)
        def _():
            @pl.when(t + LEAD == CHUNKS - 1 - FIRST)
            def _():
                for c in zc:
                    c.wait_recv()

                @pl.when(rng == 0)
                def _():
                    child[:, 0:RIM, :] = jnp.zeros((2, RIM, BEAM), F32)

                @pl.when(rng == 3)
                def _():
                    child[:, RIM + ROWS :, :] = jnp.zeros((2, RIM, BEAM), F32)

            produce(t + LEAD)
            edge_copy(t + LEAD).start()

        consume(t, jnp.where(jnp.logical_or(t == 0, j == 0), 2, 0), CHUNK // SUB)

        @pl.when(j == 0)
        def _():
            zp[0].start()

        @pl.when(j == CHUNKS - 1)
        def _():
            zp[1].start()

        whole = jnp.logical_and(t > 1, jnp.logical_and(j != 0, j != 1))

        @pl.when(whole)
        def _():
            put(j - 1).start()

        return carry

    lax.fori_loop(0, CHUNKS - 1, step, 0)

    for c in zp:
        c.wait_recv()

    @pl.when(rng == 0)
    def _():
        parent[:, TOP - RIM : TOP, :] = jnp.zeros((4, RIM, BEAM), F32)

    @pl.when(rng == 3)
    def _():
        parent[:, TOP + ROWS : TOP + ROWS + RIM, :] = jnp.zeros((4, RIM, BEAM), F32)

    ends = ((0, 0, RIM), (ROWS - RIM, CHUNKS, 0))
    for n, (first, j, rho) in enumerate(ends):
        for e in range(2):
            for half in range(2):
                fine_two(first - RIM + half * SUB, half * SUB, e, weights_two(e))
            coarse_two(n * SUB, 0, e, picks_of(step2.at[e]))
    products(len(ends) * SUB)
    for n, (first, j, rho) in enumerate(ends):
        finish(first, n * SUB, j, rho)

    put(0).start()
    put(CHUNKS - 1).start()
    consume(CHUNKS - 1, 0, CHUNK // SUB + 2)
    put(FIRST - 2).start()
    put(FIRST - 1).start()
    put(FIRST).start()

    for c in zc + zp:
        c.wait_send()

    def drain(t, carry):
        put(t).wait()
        edge_copy(t).wait_send()
        for d in (1, 3, 2):
            window_copy(t, d).wait_send()
        return carry

    lax.fori_loop(0, CHUNKS, drain, 0)


def body(*args):
    dma = pltpu.SemaphoreType.DMA
    return pl.pallas_call(
        kernel,
        out_shape=jax.ShapeDtypeStruct((1, 2, ROWS, BEAM), F32),
        in_specs=[pl.BlockSpec(memory_space=pl.ANY)] * 13,
        out_specs=pl.BlockSpec(memory_space=pl.ANY),
        scratch_shapes=[pltpu.VMEM(a.shape, a.dtype) for a in args[1:]]
        + [
            pltpu.VMEM((2, ROWS + 2 * RIM, BEAM), F32),
            pltpu.VMEM((2, CHUNK, BEAM), F32),
            pltpu.VMEM((2, BEAM + 16, ROWS), F32),
            pltpu.VMEM((4, 2, WIN, ROWS), F32),
            pltpu.VMEM((8, NEAR, BEAM), F32),
            pltpu.VMEM((4, TOP + ROWS + 32, BEAM), F32),
            pltpu.VMEM((4, NEAR, 2 * BEAM), BF16),
            pltpu.VMEM((2, ROWS, BEAM), F32),
            pltpu.VMEM((FINE, 8, BEAM), F32),
            pltpu.VMEM((2, FINE, 8, BEAM), F32),
            pltpu.VMEM((8, BEAM), jnp.int32),
            pltpu.VMEM((2, 8, BEAM), jnp.int32),
            pltpu.VMEM((4, NEAR + SUB, BEAM), F32),
            pltpu.VMEM((2, 3 * WIN, BEAM), BF16),
            pltpu.VMEM((2, 2 * BEAM, BEAM), BF16),
            pltpu.VMEM((2, BEAM, BEAM), BF16),
            pltpu.VMEM((4, NEAR, BEAM), F32),
            pltpu.VMEM((4, NEAR, BEAM), F32),
            pltpu.VMEM((4, FAR, BEAM), F32),
            pltpu.VMEM((4, FAR, BEAM), F32),
            pltpu.VMEM((24, BEAM), F32),
            pltpu.VMEM((24, BEAM), F32),
            dma((3,)),
            dma((CHUNKS,)),
            dma((12,)),
            pltpu.SemaphoreType.REGULAR,
            pltpu.SemaphoreType.REGULAR,
            dma((2,)),
            dma((2,)),
            dma((2,)),
            dma((2,)),
            dma((CHUNKS,)),
            dma((CHUNKS,)),
            dma((3, CHUNKS)),
            dma((3, CHUNKS)),
        ],
        compiler_params=pltpu.CompilerParams(
            collective_id=0, has_side_effects=True, vmem_limit_bytes=60 * 2**20
        ),
        name="merge",
    )(*args)


def solution(mesh):
    return jax.shard_map(
        body,
        mesh=mesh,
        in_specs=(P("aper", None, "rng", "beam"),) + (P(),) * 12,
        out_specs=P("aper", None, "rng", "beam"),
        check_vma=False,
    )
```

```python
import functools

import jax
import jax.numpy as jnp
from jax import lax
from jax.experimental import pallas as pl
from jax.experimental.pallas import tpu as pltpu
from jax.sharding import PartitionSpec as P

MESH = pl.DeviceIdType.MESH
ROWS = 2048
BEAM = 128
CHUNK = 128
CHUNKS = ROWS // CHUNK
FIRST = 7
EARLY = 1
LEAD = 6
NEAR = CHUNK + 32
FAR = 24
WIN = 48
TAPS = 8
FINE = 12
COARSE = 4
RIM = 16
TOP = 32
SUB = 16
F32 = jnp.float32
BF16 = jnp.bfloat16


def split_bf16(x):
    hi = x.astype(BF16)
    lo = (x - hi.astype(F32)).astype(BF16)
    return hi, lo


def range_table(shift_row, tap_rows, out_ref, step_ref):
    shift = shift_row + 8
    q = jnp.minimum(lax.shift_right_logical(shift, 2), COARSE - 1)
    p = shift - 4 * q
    step_ref[...] = jnp.broadcast_to(q, (8, BEAM))
    for o in range(FINE):
        acc = jnp.zeros((1, BEAM), F32)
        for k in range(TAPS):
            acc = acc + jnp.where(p + k == o, tap_rows[k : k + 1], 0.0)
        out_ref[o] = jnp.broadcast_to(acc, (8, BEAM))


def fine_rows(src, comps, first, weights, dst, slot):
    for n, comp in enumerate(comps):
        for v in range(2):
            acc = None
            for o in range(FINE):
                term = weights[o] * src[comp, pl.ds(first + (o + 8 * v), 8), :]
                acc = term if acc is None else acc + term
            dst[n, pl.ds(pl.multiple_of(slot + 8 * v, 8), 8), :] = acc


def coarse_rows(src, comp, slot, picks):
    out = []
    for v in range(2):
        rows = [src[comp, pl.ds(slot + (4 * q + 8 * v), 8), :] for q in range(COARSE)]
        low = jnp.where(picks[0], rows[0], rows[1])
        high = jnp.where(picks[2], rows[2], rows[3])
        out.append(jnp.where(picks[1], low, high))
    return out


def picks_of(step_ref):
    q = step_ref[...]
    return [q == 0, q < 2, q == 2]


def beam_matrix(rows, start_row, tap_rows):
    ids = lax.broadcasted_iota(jnp.int32, (rows, BEAM), 0)
    acc = jnp.zeros((rows, BEAM), F32)
    for k in range(TAPS):
        acc = acc + jnp.where(ids == start_row + k, tap_rows[k : k + 1], 0.0)
    return acc


def phase_tables(rate, off, base, lead, near_c, near_s, far_c, far_s, tmp_c, tmp_s):
    scale = 1.0 / 8192.0
    r8 = lax.broadcasted_iota(jnp.int32, (8, BEAM), 0).astype(F32) * scale
    r24 = (lax.broadcasted_iota(jnp.int32, (24, BEAM), 0) * 8).astype(F32) * scale
    rows = base + lax.broadcasted_iota(jnp.int32, (FAR, BEAM), 0) * CHUNK - lead
    far = rate * (rows.astype(F32) * scale) + off
    far_c[...] = jnp.cos(far)
    far_s[...] = jnp.sin(far)
    small = rate * r8
    sc, ss = jnp.cos(small), jnp.sin(small)
    big = rate * r24
    tmp_c[...] = jnp.cos(big)
    tmp_s[...] = jnp.sin(big)

    def fill(q, carry):
        bc = tmp_c[pl.ds(q, 1), :]
        bs = tmp_s[pl.ds(q, 1), :]
        at = pl.ds(pl.multiple_of(q * 8, 8), 8)
        near_c[at, :] = bc * sc - bs * ss
        near_s[at, :] = bs * sc + bc * ss
        return carry

    lax.fori_loop(0, NEAR // 8, fill, 0)


def kernel(
    child_hbm,
    sh1_hbm,
    rt1_hbm,
    bs1_hbm,
    bt1_hbm,
    pr1_hbm,
    po1_hbm,
    sh2_hbm,
    rt2_hbm,
    bs2_hbm,
    bt2_hbm,
    pr2_hbm,
    po2_hbm,
    image,
    sh1,
    rt1,
    bs1,
    bt1,
    pr1,
    po1,
    sh2,
    rt2,
    bs2,
    bt2,
    pr2,
    po2,
    child,
    wide,
    turned,
    got,
    mixed,
    parent,
    packed,
    tab1,
    tab2,
    step1,
    step2,
    fine,
    mat1,
    mat2a,
    mat2b,
    near_c,
    near_s,
    far_c,
    far_s,
    tmp_c,
    tmp_s,
    in_sem,
    tab_sem,
    chip_sem,
    core_sem,
    zs_sem,
    zr_sem,
    ps_sem,
    pr_sem,
    es_sem,
    er_sem,
    xs_sem,
    xr_sem,
):
    aper = lax.axis_index("aper")
    rng = lax.axis_index("rng")
    beam = lax.axis_index("beam")
    me = lax.rem(aper, 4)
    group = aper - me
    block = 4 * beam + me
    up, down = lax.rem(rng + 3, 4), lax.rem(rng + 1, 4)

    def peer(d):
        return lax.rem(me + d, 4)

    def chunk_of(t):
        return lax.rem(t + FIRST, CHUNKS)

    cut = (0, FIRST * CHUNK - RIM, (FIRST + EARLY) * CHUNK + RIM, ROWS)
    loads = [
        pltpu.make_async_copy(
            child_hbm.at[0, :, pl.ds(cut[n], cut[n + 1] - cut[n]), :],
            child.at[:, pl.ds(RIM + cut[n], cut[n + 1] - cut[n]), :],
            in_sem.at[n],
        )
        for n in (1, 2, 0)
    ]
    tables = [
        pltpu.make_async_copy(src, dst, tab_sem.at[n])
        for n, (src, dst) in enumerate(
            (
                (sh1_hbm, sh1),
                (rt1_hbm, rt1),
                (bs1_hbm, bs1),
                (bt1_hbm, bt1),
                (pr1_hbm, pr1),
                (po1_hbm, po1),
                (sh2_hbm, sh2),
                (rt2_hbm, rt2),
                (bs2_hbm, bs2),
                (bt2_hbm, bt2),
                (pr2_hbm, pr2),
                (po2_hbm, po2),
            )
        )
    ]
    for c in tables[:2]:
        c.start()
    for c in loads:
        c.start()
    for c in tables[2:]:
        c.start()

    barrier = pltpu.get_barrier_semaphore()
    partner = (aper, rng, 1 - beam)

    @pl.when(beam == 0)
    def _():
        for d in (1, 2, 3):
            pl.semaphore_signal(
                barrier, inc=1, device_id=(group + peer(d), rng, beam), device_id_type=MESH
            )

    @pl.when(beam == 1)
    def _():
        pl.semaphore_signal(barrier, inc=1, device_id=partner, device_id_type=MESH)

    @pl.when(beam == 0)
    def _():
        pl.semaphore_wait(barrier, 4)
        for d in (1, 2, 3):
            pl.semaphore_signal(
                chip_sem, inc=1, device_id=(group + peer(d), rng, beam), device_id_type=MESH
            )

    @pl.when(beam == 0)
    def _():
        turned[:, 0:8, :] = jnp.zeros((2, 8, ROWS), F32)

    @pl.when(beam == 1)
    def _():
        turned[:, 136:144, :] = jnp.zeros((2, 8, ROWS), F32)

    for c in tables[:2]:
        c.wait()
    side = lax.div(me, 2)
    own = pl.ds(pl.multiple_of(beam * BEAM, BEAM), BEAM)
    shift_row = jnp.where(side == 0, sh1[0:1, own], sh1[1:2, own])
    range_table(shift_row, rt1[side, :, own], tab1, step1)

    def halo(buf, sem_s, sem_r, first, last, low, high):
        return (
            pltpu.make_async_remote_copy(
                src_ref=buf.at[:, pl.ds(first, RIM), :],
                dst_ref=buf.at[:, pl.ds(high, RIM), :],
                send_sem=sem_s.at[0],
                recv_sem=sem_r.at[0],
                device_id=(aper, up, beam),
                device_id_type=MESH,
            ),
            pltpu.make_async_remote_copy(
                src_ref=buf.at[:, pl.ds(last, RIM), :],
                dst_ref=buf.at[:, pl.ds(low, RIM), :],
                send_sem=sem_s.at[1],
                recv_sem=sem_r.at[1],
                device_id=(aper, down, beam),
                device_id_type=MESH,
            ),
        )

    zc = halo(child, zs_sem, zr_sem, RIM, ROWS, 0, RIM + ROWS)
    zp = halo(parent, ps_sem, pr_sem, TOP, TOP + ROWS - RIM, TOP - RIM, TOP + ROWS)

    def edge_copy(t):
        at = pl.ds(pl.multiple_of(chunk_of(t) * CHUNK, CHUNK), CHUNK)
        return pltpu.make_async_remote_copy(
            src_ref=turned.at[:, pl.ds(pl.multiple_of(128 - 120 * beam, 8), 8), at],
            dst_ref=turned.at[:, pl.ds(pl.multiple_of(136 * beam, 8), 8), at],
            send_sem=es_sem.at[t],
            recv_sem=er_sem.at[t],
            device_id=(aper, rng, 1 - beam),
            device_id_type=MESH,
        )

    def window_copy(t, d):
        at = pl.ds(pl.multiple_of(chunk_of(t) * CHUNK, CHUNK), CHUNK)
        to = peer(d)
        return pltpu.make_async_remote_copy(
            src_ref=turned.at[:, pl.ds(pl.multiple_of(32 * to, 8), WIN), at],
            dst_ref=got.at[me, :, :, at],
            send_sem=xs_sem.at[d - 1, t],
            recv_sem=xr_sem.at[d - 1, t],
            device_id=(group + to, rng, beam),
            device_id_type=MESH,
        )

    def produce(t):
        j = chunk_of(t)
        base = pl.multiple_of(j * CHUNK, CHUNK)

        weights = [tab1[o] for o in range(FINE)]
        picks = picks_of(step1)

        def fine_in(s, carry):
            slot = pl.multiple_of(s * SUB, SUB)
            fine_rows(child, (0, 1), base + (RIM - 16) + slot, weights, fine, slot)
            return carry

        def coarse_in(s, carry):
            slot = pl.multiple_of(s * SUB, SUB)
            for comp in range(2):
                for v, x in enumerate(coarse_rows(fine, comp, slot + 4, picks)):
                    wide[comp, pl.ds(pl.multiple_of(slot + 8 * v, 8), 8), :] = x
            return carry

        lax.fori_loop(0, CHUNK // SUB + 1, fine_in, 0)
        lax.fori_loop(0, CHUNK // SUB, coarse_in, 0)
        for comp in range(2):
            for half in range(CHUNK // BEAM):
                turned[
                    comp, 8:136, pl.ds(pl.multiple_of(base + half * BEAM, BEAM), BEAM)
                ] = jnp.transpose(wide[comp, half * BEAM : (half + 1) * BEAM, :])

    def inner(d):
        return jnp.logical_or(peer(d) == 1, peer(d) == 2)

    def send(t):
        edge_copy(t).wait_recv()
        for d in (1, 3, 2):
            window_copy(t, d).start()
        keep(t)

    def keep(t):
        at = pl.ds(pl.multiple_of(chunk_of(t) * CHUNK, CHUNK), CHUNK)
        got[me, :, :, at] = turned[:, pl.ds(pl.multiple_of(32 * me, 8), WIN), at]

    loads[0].wait()
    produce(0)

    def open_windows():
        edge_copy(0).start()
        for d in (1, 3, 2):

            @pl.when(inner(d))
            def _(d=d):
                window_copy(0, d).start()

    @pl.when(beam == 0)
    def _():
        open_windows()
        pl.semaphore_wait(chip_sem, 3)
        pl.semaphore_signal(core_sem, inc=1, device_id=partner, device_id_type=MESH)

    @pl.when(beam == 1)
    def _():
        pl.semaphore_wait(core_sem, 1)
        for z in (up, down):
            pl.semaphore_signal(barrier, inc=1, device_id=(aper, z, beam), device_id_type=MESH)
        open_windows()

    loads[1].wait()
    produce(1)
    edge_copy(1).start()
    edge_copy(0).wait_recv()
    for d in (1, 3, 2):

        @pl.when(jnp.logical_not(inner(d)))
        def _(d=d):
            window_copy(0, d).start()

    keep(0)
    loads[2].wait()

    def lead_step(t, carry):
        produce(t)
        edge_copy(t).start()
        send(t - 1)
        return carry

    lax.fori_loop(2, LEAD, lead_step, 0)

    @pl.when(beam == 1)
    def _():
        pl.semaphore_wait(barrier, 2)
        pl.semaphore_signal(core_sem, inc=1, device_id=partner, device_id_type=MESH)

    @pl.when(beam == 0)
    def _():
        pl.semaphore_wait(core_sem, 1)

    for c in zc:
        c.start()

    for c in tables[2:]:
        c.wait()
    shift = lax.rem(520 - 64 * block, 512)

    def lanes(v):
        return pltpu.roll(v, shift, 1)[:, :BEAM]

    ints = lanes(jnp.concatenate([bs1[...], sh2[...], bs1[...], sh2[...]], axis=0))
    floats = lanes(jnp.concatenate([pr1[...], po1[...], pr1[...], po1[...]], axis=0))
    beams_here = lax.broadcasted_iota(jnp.int32, (TAPS, BEAM), 1) + (64 * block - 8)
    inside = jnp.logical_and(beams_here >= 0, beams_here < 512)
    final = pl.ds(pl.multiple_of(block * BEAM, BEAM), BEAM)
    for s in range(2):
        taps = jnp.where(inside, lanes(bt1[s]), 0.0)
        m = beam_matrix(WIN, ints[s : s + 1] - (32 * block - 8), taps)
        hi, lo = split_bf16(m)
        mat1[s, 0:WIN, :] = hi
        mat1[s, WIN : 2 * WIN, :] = hi
        mat1[s, 2 * WIN : 3 * WIN, :] = lo
        range_table(ints[2 + s : 3 + s], lanes(rt2[s]), tab2.at[s], step2.at[s])
        m = beam_matrix(BEAM, bs2[s : s + 1, final] - (64 * block - 8), bt2[s, :, final])
        hi, lo = split_bf16(m)
        mat2a[s, 0:BEAM, :] = hi
        mat2a[s, BEAM : 2 * BEAM, :] = hi
        mat2b[s] = lo
        phase_tables(
            floats[s : s + 1],
            floats[2 + s : 3 + s],
            rng * ROWS,
            0,
            near_c.at[s],
            near_s.at[s],
            far_c.at[s],
            far_s.at[s],
            tmp_c,
            tmp_s,
        )
        phase_tables(
            pr2[s : s + 1, final],
            po2[s : s + 1, final],
            rng * ROWS,
            RIM,
            near_c.at[2 + s],
            near_s.at[2 + s],
            far_c.at[2 + s],
            far_s.at[2 + s],
            tmp_c,
            tmp_s,
        )

    def turn(level, j, rho):
        both = []
        for s in range(2):
            fc = far_c[2 * level + s, pl.ds(j, 1), :]
            fs = far_s[2 * level + s, pl.ds(j, 1), :]
            nc = near_c[2 * level + s, pl.ds(rho, SUB), :]
            ns = near_s[2 * level + s, pl.ds(rho, SUB), :]
            both.append((fc * nc - fs * ns, fs * nc + fc * ns))
        return both

    def make_parents(j):
        at = pl.ds(pl.multiple_of(j * CHUNK, CHUNK), CHUNK)
        for c in range(4):
            both = jnp.concatenate([got[c, 0, :, at], got[c, 1, :, at]], axis=1)
            hi, lo = split_bf16(both)
            mixed[2 * c : 2 * c + 2, 0:CHUNK, :] = lax.dot_general(
                jnp.concatenate([hi, lo, hi], axis=0),
                mat1[c // 2],
                (((0,), (0,)), ((), ())),
                preferred_element_type=F32,
            ).reshape(2, CHUNK, BEAM)

        def rows(s, carry):
            rho = pl.multiple_of(s * SUB, SUB)
            (c0, s0), (c1, s1) = turn(0, j, rho)
            here = pl.ds(rho, SUB)
            to = pl.ds(pl.multiple_of(TOP + j * CHUNK + rho, SUB), SUB)
            for e in range(2):
                lr, li = mixed[2 * e, here, :], mixed[2 * e + 1, here, :]
                rr, ri = mixed[4 + 2 * e, here, :], mixed[5 + 2 * e, here, :]
                parent[2 * e, to, :] = (c0 * lr - s0 * li) + (c1 * rr - s1 * ri)
                parent[2 * e + 1, to, :] = (s0 * lr + c0 * li) + (s1 * rr + c1 * ri)
            return carry

        lax.fori_loop(0, CHUNK // SUB, rows, 0)

    def fine_two(first, slot, e, weights):
        fine_rows(
            parent, (2 * e, 2 * e + 1), first + TOP, weights, fine.at[pl.ds(2 * e, 2)], slot
        )

    def coarse_two(slot, from_slot, e, picks):
        for comp in range(2):
            rows = coarse_rows(fine, 2 * e + comp, from_slot + 4, picks)
            hi, lo = split_bf16(jnp.concatenate(rows, axis=0))
            packed[2 * e + comp, pl.ds(slot, SUB), 0:BEAM] = hi
            packed[2 * e + comp, pl.ds(slot, SUB), BEAM : 2 * BEAM] = lo

    def weights_two(e):
        return [tab2[e, o] for o in range(FINE)]

    def products(count):
        for e in range(2):
            z = packed[2 * e : 2 * e + 2, 0:count, :].reshape(2 * count, 2 * BEAM)
            mixed[2 * e : 2 * e + 2, 0:count, :] = (
                jnp.dot(z, mat2a[e], preferred_element_type=F32)
                + jnp.dot(z[:, :BEAM], mat2b[e], preferred_element_type=F32)
            ).reshape(2, count, BEAM)

    def finish(first, slot, j, rho):
        (c0, s0), (c1, s1) = turn(1, j, rho)
        here = pl.ds(slot, SUB)
        to = pl.ds(first, SUB)
        lr, li, rr, ri = (mixed[i, here, :] for i in range(4))
        image[0, 0, to, :] = (c0 * lr - s0 * li) + (c1 * rr - s1 * ri)
        image[0, 1, to, :] = (s0 * lr + c0 * li) + (s1 * rr + c1 * ri)

    def consume(t, begin, end):
        j = chunk_of(t)
        for d in (1, 3, 2):
            window_copy(t, d).wait_recv()
        make_parents(j)

        def fine_in(s, carry, e, weights):
            slot = pl.multiple_of(s * SUB, SUB)
            fine_two(j * CHUNK - 2 * RIM + slot, slot, e, weights)
            return carry

        def coarse_in(s, carry, e, picks):
            slot = pl.multiple_of(s * SUB, SUB)
            coarse_two(slot, slot, e, picks)
            return carry

        def rows_out(s, carry):
            slot = pl.multiple_of(s * SUB, SUB)
            finish(pl.multiple_of(j * CHUNK - RIM + slot, SUB), slot, j, slot)
            return carry

        for e in range(2):
            lax.fori_loop(
                begin, end + 1, functools.partial(fine_in, e=e, weights=weights_two(e)), 0
            )
            lax.fori_loop(
                begin, end, functools.partial(coarse_in, e=e, picks=picks_of(step2.at[e])), 0
            )
        products(end * SUB)
        lax.fori_loop(begin, end, rows_out, 0)

    def step(t, carry):
        j = chunk_of(t)

        @pl.when(t + LEAD - 1 < CHUNKS)
        def _():
            send(t + LEAD - 1)

        @pl.when(t + LEAD < CHUNKS)
        def _():
            @pl.when(t + LEAD == CHUNKS - 1 - FIRST)
            def _():
                for c in zc:
                    c.wait_recv()

                @pl.when(rng == 0)
                def _():
                    child[:, 0:RIM, :] = jnp.zeros((2, RIM, BEAM), F32)

                @pl.when(rng == 3)
                def _():
                    child[:, RIM + ROWS :, :] = jnp.zeros((2, RIM, BEAM), F32)

            produce(t + LEAD)
            edge_copy(t + LEAD).start()

        consume(t, jnp.where(jnp.logical_or(t == 0, j == 0), 2, 0), CHUNK // SUB)

        @pl.when(j == 0)
        def _():
            zp[0].start()

        @pl.when(j == CHUNKS - 1)
        def _():
            zp[1].start()

        return carry

    lax.fori_loop(0, CHUNKS - 1, step, 0)

    for c in zp:
        c.wait_recv()

    @pl.when(rng == 0)
    def _():
        parent[:, TOP - RIM : TOP, :] = jnp.zeros((4, RIM, BEAM), F32)

    @pl.when(rng == 3)
    def _():
        parent[:, TOP + ROWS : TOP + ROWS + RIM, :] = jnp.zeros((4, RIM, BEAM), F32)

    ends = ((0, 0, RIM), (ROWS - RIM, CHUNKS, 0))
    for n, (first, j, rho) in enumerate(ends):
        for e in range(2):
            for half in range(2):
                fine_two(first - RIM + half * SUB, half * SUB, e, weights_two(e))
            coarse_two(n * SUB, 0, e, picks_of(step2.at[e]))
    products(len(ends) * SUB)
    for n, (first, j, rho) in enumerate(ends):
        finish(first, n * SUB, j, rho)

    consume(CHUNKS - 1, 0, CHUNK // SUB + 2)

    for c in zc + zp:
        c.wait_send()

    def drain(t, carry):
        edge_copy(t).wait_send()
        for d in (1, 3, 2):
            window_copy(t, d).wait_send()
        return carry

    lax.fori_loop(0, CHUNKS, drain, 0)


def body(*args):
    dma = pltpu.SemaphoreType.DMA
    args = [pltpu.with_memory_space_constraint(a, pltpu.HBM) for a in args]
    return pl.pallas_call(
        kernel,
        out_shape=jax.ShapeDtypeStruct((1, 2, ROWS, BEAM), F32),
        in_specs=[pl.BlockSpec(memory_space=pl.ANY)] * 13,
        out_specs=pl.BlockSpec(memory_space=pltpu.VMEM),
        scratch_shapes=[pltpu.VMEM(a.shape, a.dtype) for a in args[1:]]
        + [
            pltpu.VMEM((2, ROWS + 2 * RIM, BEAM), F32),
            pltpu.VMEM((2, CHUNK, BEAM), F32),
            pltpu.VMEM((2, BEAM + 16, ROWS), F32),
            pltpu.VMEM((4, 2, WIN, ROWS), F32),
            pltpu.VMEM((8, NEAR, BEAM), F32),
            pltpu.VMEM((4, TOP + ROWS + 32, BEAM), F32),
            pltpu.VMEM((4, NEAR, 2 * BEAM), BF16),
            pltpu.VMEM((FINE, 8, BEAM), F32),
            pltpu.VMEM((2, FINE, 8, BEAM), F32),
            pltpu.VMEM((8, BEAM), jnp.int32),
            pltpu.VMEM((2, 8, BEAM), jnp.int32),
            pltpu.VMEM((4, NEAR + SUB, BEAM), F32),
            pltpu.VMEM((2, 3 * WIN, BEAM), BF16),
            pltpu.VMEM((2, 2 * BEAM, BEAM), BF16),
            pltpu.VMEM((2, BEAM, BEAM), BF16),
            pltpu.VMEM((4, NEAR, BEAM), F32),
            pltpu.VMEM((4, NEAR, BEAM), F32),
            pltpu.VMEM((4, FAR, BEAM), F32),
            pltpu.VMEM((4, FAR, BEAM), F32),
            pltpu.VMEM((24, BEAM), F32),
            pltpu.VMEM((24, BEAM), F32),
            dma((3,)),
            dma((12,)),
            pltpu.SemaphoreType.REGULAR,
            pltpu.SemaphoreType.REGULAR,
            dma((2,)),
            dma((2,)),
            dma((2,)),
            dma((2,)),
            dma((CHUNKS,)),
            dma((CHUNKS,)),
            dma((3, CHUNKS)),
            dma((3, CHUNKS)),
        ],
        compiler_params=pltpu.CompilerParams(
            collective_id=0, has_side_effects=True, vmem_limit_bytes=36 * 2**20
        ),
        name="merge",
    )(*args)


def solution(mesh):
    return jax.shard_map(
        body,
        mesh=mesh,
        in_specs=(P("aper", None, "rng", "beam"),) + (P(),) * 12,
        out_specs=P("aper", None, "rng", "beam"),
        check_vma=False,
    )
```

```python
import functools

import jax
import jax.numpy as jnp
from jax import lax
from jax.experimental import pallas as pl
from jax.experimental.pallas import tpu as pltpu
from jax.sharding import PartitionSpec as P

MESH = pl.DeviceIdType.MESH
ROWS = 2048
BEAM = 128
CHUNK = 128
CHUNKS = ROWS // CHUNK
FIRST = 7
EARLY = 1
LEAD = 6
NEAR = CHUNK + 32
FAR = 24
WIN = 48
TAPS = 8
FINE = 12
COARSE = 4
RIM = 16
TOP = 32
SUB = 16
F32 = jnp.float32
BF16 = jnp.bfloat16


def split_bf16(x):
    hi = x.astype(BF16)
    lo = (x - hi.astype(F32)).astype(BF16)
    return hi, lo


def range_table(shift_row, tap_rows, out_ref, step_ref):
    shift = shift_row + 8
    q = jnp.minimum(lax.shift_right_logical(shift, 2), COARSE - 1)
    p = shift - 4 * q
    step_ref[...] = jnp.broadcast_to(q, (8, BEAM))
    for o in range(FINE):
        acc = jnp.zeros((1, BEAM), F32)
        for k in range(TAPS):
            acc = acc + jnp.where(p + k == o, tap_rows[k : k + 1], 0.0)
        out_ref[o] = jnp.broadcast_to(acc, (8, BEAM))


def fine_rows(src, comps, first, weights, dst, slot):
    for n, comp in enumerate(comps):
        for v in range(2):
            acc = None
            for o in range(FINE):
                term = weights[o] * src[comp, pl.ds(first + (o + 8 * v), 8), :]
                acc = term if acc is None else acc + term
            dst[n, pl.ds(pl.multiple_of(slot + 8 * v, 8), 8), :] = acc


def coarse_rows(src, comp, slot, picks):
    out = []
    for v in range(2):
        rows = [src[comp, pl.ds(slot + (4 * q + 8 * v), 8), :] for q in range(COARSE)]
        low = jnp.where(picks[0], rows[0], rows[1])
        high = jnp.where(picks[2], rows[2], rows[3])
        out.append(jnp.where(picks[1], low, high))
    return out


def picks_of(step_ref):
    q = step_ref[...]
    return [q == 0, q < 2, q == 2]


def beam_matrix(rows, start_row, tap_rows):
    ids = lax.broadcasted_iota(jnp.int32, (rows, BEAM), 0)
    acc = jnp.zeros((rows, BEAM), F32)
    for k in range(TAPS):
        acc = acc + jnp.where(ids == start_row + k, tap_rows[k : k + 1], 0.0)
    return acc


def phase_tables(rate, off, base, lead, near_c, near_s, far_c, far_s, tmp_c, tmp_s):
    scale = 1.0 / 8192.0
    r8 = lax.broadcasted_iota(jnp.int32, (8, BEAM), 0).astype(F32) * scale
    r24 = (lax.broadcasted_iota(jnp.int32, (24, BEAM), 0) * 8).astype(F32) * scale
    rows = base + lax.broadcasted_iota(jnp.int32, (FAR, BEAM), 0) * CHUNK - lead
    far = rate * (rows.astype(F32) * scale) + off
    far_c[...] = jnp.cos(far)
    far_s[...] = jnp.sin(far)
    small = rate * r8
    sc, ss = jnp.cos(small), jnp.sin(small)
    big = rate * r24
    tmp_c[...] = jnp.cos(big)
    tmp_s[...] = jnp.sin(big)

    def fill(q, carry):
        bc = tmp_c[pl.ds(q, 1), :]
        bs = tmp_s[pl.ds(q, 1), :]
        at = pl.ds(pl.multiple_of(q * 8, 8), 8)
        near_c[at, :] = bc * sc - bs * ss
        near_s[at, :] = bs * sc + bc * ss
        return carry

    lax.fori_loop(0, NEAR // 8, fill, 0)


def kernel(
    child_hbm,
    sh1_hbm,
    rt1_hbm,
    bs1_hbm,
    bt1_hbm,
    pr1_hbm,
    po1_hbm,
    sh2_hbm,
    rt2_hbm,
    bs2_hbm,
    bt2_hbm,
    pr2_hbm,
    po2_hbm,
    image,
    sh1,
    rt1,
    bs1,
    bt1,
    pr1,
    po1,
    sh2,
    rt2,
    bs2,
    bt2,
    pr2,
    po2,
    child,
    wide,
    turned,
    got,
    mixed,
    parent,
    packed,
    tab1,
    tab2,
    step1,
    step2,
    fine,
    mat1,
    mat2a,
    mat2b,
    near_c,
    near_s,
    far_c,
    far_s,
    tmp_c,
    tmp_s,
    in_sem,
    tab_sem,
    chip_sem,
    core_sem,
    zs_sem,
    zr_sem,
    ps_sem,
    pr_sem,
    es_sem,
    er_sem,
    xs_sem,
    xr_sem,
):
    aper = lax.axis_index("aper")
    rng = lax.axis_index("rng")
    beam = lax.axis_index("beam")
    me = lax.rem(aper, 4)
    group = aper - me
    block = 4 * beam + me
    up, down = lax.rem(rng + 3, 4), lax.rem(rng + 1, 4)

    def peer(d):
        return lax.rem(me + d, 4)

    def chunk_of(t):
        return lax.rem(t + FIRST, CHUNKS)

    cut = (0, FIRST * CHUNK - RIM, (FIRST + EARLY) * CHUNK + RIM, ROWS)
    loads = [
        pltpu.make_async_copy(
            child_hbm.at[0, :, pl.ds(cut[n], cut[n + 1] - cut[n]), :],
            child.at[:, pl.ds(RIM + cut[n], cut[n + 1] - cut[n]), :],
            in_sem.at[n],
        )
        for n in (1, 2, 0)
    ]
    tables = [
        pltpu.make_async_copy(src, dst, tab_sem.at[n])
        for n, (src, dst) in enumerate(
            (
                (sh1_hbm, sh1),
                (rt1_hbm, rt1),
                (bs1_hbm, bs1),
                (bt1_hbm, bt1),
                (pr1_hbm, pr1),
                (po1_hbm, po1),
                (sh2_hbm, sh2),
                (rt2_hbm, rt2),
                (bs2_hbm, bs2),
                (bt2_hbm, bt2),
                (pr2_hbm, pr2),
                (po2_hbm, po2),
            )
        )
    ]
    for c in tables[:2]:
        c.start()
    for c in loads:
        c.start()
    for c in tables[2:]:
        c.start()

    barrier = pltpu.get_barrier_semaphore()
    partner = (aper, rng, 1 - beam)

    @pl.when(beam == 0)
    def _():
        for d in (1, 2, 3):
            pl.semaphore_signal(
                barrier, inc=1, device_id=(group + peer(d), rng, beam), device_id_type=MESH
            )

    @pl.when(beam == 1)
    def _():
        pl.semaphore_signal(barrier, inc=1, device_id=partner, device_id_type=MESH)

    @pl.when(beam == 0)
    def _():
        pl.semaphore_wait(barrier, 4)
        for d in (1, 2, 3):
            pl.semaphore_signal(
                chip_sem, inc=1, device_id=(group + peer(d), rng, beam), device_id_type=MESH
            )

    @pl.when(beam == 0)
    def _():
        turned[:, 0:8, :] = jnp.zeros((2, 8, ROWS), F32)

    @pl.when(beam == 1)
    def _():
        turned[:, 136:144, :] = jnp.zeros((2, 8, ROWS), F32)

    for c in tables[:2]:
        c.wait()
    side = lax.div(me, 2)
    own = pl.ds(pl.multiple_of(beam * BEAM, BEAM), BEAM)
    shift_row = jnp.where(side == 0, sh1[0:1, own], sh1[1:2, own])
    range_table(shift_row, rt1[side, :, own], tab1, step1)

    def halo(buf, sem_s, sem_r, first, last, low, high):
        return (
            pltpu.make_async_remote_copy(
                src_ref=buf.at[:, pl.ds(first, RIM), :],
                dst_ref=buf.at[:, pl.ds(high, RIM), :],
                send_sem=sem_s.at[0],
                recv_sem=sem_r.at[0],
                device_id=(aper, up, beam),
                device_id_type=MESH,
            ),
            pltpu.make_async_remote_copy(
                src_ref=buf.at[:, pl.ds(last, RIM), :],
                dst_ref=buf.at[:, pl.ds(low, RIM), :],
                send_sem=sem_s.at[1],
                recv_sem=sem_r.at[1],
                device_id=(aper, down, beam),
                device_id_type=MESH,
            ),
        )

    zc = halo(child, zs_sem, zr_sem, RIM, ROWS, 0, RIM + ROWS)
    zp = halo(parent, ps_sem, pr_sem, TOP, TOP + ROWS - RIM, TOP - RIM, TOP + ROWS)

    def edge_copy(t):
        at = pl.ds(pl.multiple_of(chunk_of(t) * CHUNK, CHUNK), CHUNK)
        return pltpu.make_async_remote_copy(
            src_ref=turned.at[:, pl.ds(pl.multiple_of(128 - 120 * beam, 8), 8), at],
            dst_ref=turned.at[:, pl.ds(pl.multiple_of(136 * beam, 8), 8), at],
            send_sem=es_sem.at[t],
            recv_sem=er_sem.at[t],
            device_id=(aper, rng, 1 - beam),
            device_id_type=MESH,
        )

    def window_copy(t, d):
        at = pl.ds(pl.multiple_of(chunk_of(t) * CHUNK, CHUNK), CHUNK)
        to = peer(d)
        return pltpu.make_async_remote_copy(
            src_ref=turned.at[:, pl.ds(pl.multiple_of(32 * to, 8), WIN), at],
            dst_ref=got.at[me, :, :, at],
            send_sem=xs_sem.at[d - 1, t],
            recv_sem=xr_sem.at[d - 1, t],
            device_id=(group + to, rng, beam),
            device_id_type=MESH,
        )

    def produce(t):
        j = chunk_of(t)
        base = pl.multiple_of(j * CHUNK, CHUNK)

        weights = [tab1[o] for o in range(FINE)]
        picks = picks_of(step1)

        def fine_in(s, carry):
            slot = pl.multiple_of(s * SUB, SUB)
            fine_rows(child, (0, 1), base + (RIM - 16) + slot, weights, fine, slot)
            return carry

        def coarse_in(s, carry):
            slot = pl.multiple_of(s * SUB, SUB)
            for comp in range(2):
                for v, x in enumerate(coarse_rows(fine, comp, slot + 4, picks)):
                    wide[comp, pl.ds(pl.multiple_of(slot + 8 * v, 8), 8), :] = x
            return carry

        lax.fori_loop(0, CHUNK // SUB + 1, fine_in, 0)
        lax.fori_loop(0, CHUNK // SUB, coarse_in, 0)
        for comp in range(2):
            for half in range(CHUNK // BEAM):
                turned[
                    comp, 8:136, pl.ds(pl.multiple_of(base + half * BEAM, BEAM), BEAM)
                ] = jnp.transpose(wide[comp, half * BEAM : (half + 1) * BEAM, :])

    def inner(d):
        return jnp.logical_or(peer(d) == 1, peer(d) == 2)

    def send(t):
        edge_copy(t).wait_recv()
        for d in (2, 1, 3):
            window_copy(t, d).start()
        keep(t)

    def keep(t):
        at = pl.ds(pl.multiple_of(chunk_of(t) * CHUNK, CHUNK), CHUNK)
        got[me, :, :, at] = turned[:, pl.ds(pl.multiple_of(32 * me, 8), WIN), at]

    loads[0].wait()
    produce(0)

    def open_windows():
        edge_copy(0).start()
        for d in (2, 1, 3):

            @pl.when(inner(d))
            def _(d=d):
                window_copy(0, d).start()

    @pl.when(beam == 0)
    def _():
        open_windows()
        pl.semaphore_wait(chip_sem, 3)
        pl.semaphore_signal(core_sem, inc=1, device_id=partner, device_id_type=MESH)

    @pl.when(beam == 1)
    def _():
        pl.semaphore_wait(core_sem, 1)
        for z in (up, down):
            pl.semaphore_signal(barrier, inc=1, device_id=(aper, z, beam), device_id_type=MESH)
        open_windows()

    loads[1].wait()
    produce(1)
    edge_copy(1).start()
    edge_copy(0).wait_recv()
    for d in (2, 1, 3):

        @pl.when(jnp.logical_not(inner(d)))
        def _(d=d):
            window_copy(0, d).start()

    keep(0)
    loads[2].wait()

    def lead_step(t, carry):
        produce(t)
        edge_copy(t).start()
        send(t - 1)
        return carry

    lax.fori_loop(2, LEAD, lead_step, 0)

    @pl.when(beam == 1)
    def _():
        pl.semaphore_wait(barrier, 2)
        pl.semaphore_signal(core_sem, inc=1, device_id=partner, device_id_type=MESH)

    @pl.when(beam == 0)
    def _():
        pl.semaphore_wait(core_sem, 1)

    for c in zc:
        c.start()

    for c in tables[2:]:
        c.wait()
    shift = lax.rem(520 - 64 * block, 512)

    def lanes(v):
        return pltpu.roll(v, shift, 1)[:, :BEAM]

    ints = lanes(jnp.concatenate([bs1[...], sh2[...], bs1[...], sh2[...]], axis=0))
    floats = lanes(jnp.concatenate([pr1[...], po1[...], pr1[...], po1[...]], axis=0))
    beams_here = lax.broadcasted_iota(jnp.int32, (TAPS, BEAM), 1) + (64 * block - 8)
    inside = jnp.logical_and(beams_here >= 0, beams_here < 512)
    final = pl.ds(pl.multiple_of(block * BEAM, BEAM), BEAM)
    for s in range(2):
        taps = jnp.where(inside, lanes(bt1[s]), 0.0)
        m = beam_matrix(WIN, ints[s : s + 1] - (32 * block - 8), taps)
        hi, lo = split_bf16(m)
        mat1[s, 0:WIN, :] = hi
        mat1[s, WIN : 2 * WIN, :] = hi
        mat1[s, 2 * WIN : 3 * WIN, :] = lo
        range_table(ints[2 + s : 3 + s], lanes(rt2[s]), tab2.at[s], step2.at[s])
        m = beam_matrix(BEAM, bs2[s : s + 1, final] - (64 * block - 8), bt2[s, :, final])
        hi, lo = split_bf16(m)
        mat2a[s, 0:BEAM, :] = hi
        mat2a[s, BEAM : 2 * BEAM, :] = hi
        mat2b[s] = lo
        phase_tables(
            floats[s : s + 1],
            floats[2 + s : 3 + s],
            rng * ROWS,
            0,
            near_c.at[s],
            near_s.at[s],
            far_c.at[s],
            far_s.at[s],
            tmp_c,
            tmp_s,
        )
        phase_tables(
            pr2[s : s + 1, final],
            po2[s : s + 1, final],
            rng * ROWS,
            RIM,
            near_c.at[2 + s],
            near_s.at[2 + s],
            far_c.at[2 + s],
            far_s.at[2 + s],
            tmp_c,
            tmp_s,
        )

    def turn(level, j, rho):
        both = []
        for s in range(2):
            fc = far_c[2 * level + s, pl.ds(j, 1), :]
            fs = far_s[2 * level + s, pl.ds(j, 1), :]
            nc = near_c[2 * level + s, pl.ds(rho, SUB), :]
            ns = near_s[2 * level + s, pl.ds(rho, SUB), :]
            both.append((fc * nc - fs * ns, fs * nc + fc * ns))
        return both

    def make_parents(j):
        at = pl.ds(pl.multiple_of(j * CHUNK, CHUNK), CHUNK)
        for c in range(4):
            both = jnp.concatenate([got[c, 0, :, at], got[c, 1, :, at]], axis=1)
            hi, lo = split_bf16(both)
            mixed[2 * c : 2 * c + 2, 0:CHUNK, :] = lax.dot_general(
                jnp.concatenate([hi, lo, hi], axis=0),
                mat1[c // 2],
                (((0,), (0,)), ((), ())),
                preferred_element_type=F32,
            ).reshape(2, CHUNK, BEAM)

        def rows(s, carry):
            rho = pl.multiple_of(s * SUB, SUB)
            (c0, s0), (c1, s1) = turn(0, j, rho)
            here = pl.ds(rho, SUB)
            to = pl.ds(pl.multiple_of(TOP + j * CHUNK + rho, SUB), SUB)
            for e in range(2):
                lr, li = mixed[2 * e, here, :], mixed[2 * e + 1, here, :]
                rr, ri = mixed[4 + 2 * e, here, :], mixed[5 + 2 * e, here, :]
                parent[2 * e, to, :] = (c0 * lr - s0 * li) + (c1 * rr - s1 * ri)
                parent[2 * e + 1, to, :] = (s0 * lr + c0 * li) + (s1 * rr + c1 * ri)
            return carry

        lax.fori_loop(0, CHUNK // SUB, rows, 0)

    def fine_two(first, slot, e, weights):
        fine_rows(
            parent, (2 * e, 2 * e + 1), first + TOP, weights, fine.at[pl.ds(2 * e, 2)], slot
        )

    def coarse_two(slot, from_slot, e, picks):
        for comp in range(2):
            rows = coarse_rows(fine, 2 * e + comp, from_slot + 4, picks)
            hi, lo = split_bf16(jnp.concatenate(rows, axis=0))
            packed[2 * e + comp, pl.ds(slot, SUB), 0:BEAM] = hi
            packed[2 * e + comp, pl.ds(slot, SUB), BEAM : 2 * BEAM] = lo

    def weights_two(e):
        return [tab2[e, o] for o in range(FINE)]

    def products(count):
        for e in range(2):
            z = packed[2 * e : 2 * e + 2, 0:count, :].reshape(2 * count, 2 * BEAM)
            mixed[2 * e : 2 * e + 2, 0:count, :] = (
                jnp.dot(z, mat2a[e], preferred_element_type=F32)
                + jnp.dot(z[:, :BEAM], mat2b[e], preferred_element_type=F32)
            ).reshape(2, count, BEAM)

    def finish(first, slot, j, rho):
        (c0, s0), (c1, s1) = turn(1, j, rho)
        here = pl.ds(slot, SUB)
        to = pl.ds(first, SUB)
        lr, li, rr, ri = (mixed[i, here, :] for i in range(4))
        image[0, 0, to, :] = (c0 * lr - s0 * li) + (c1 * rr - s1 * ri)
        image[0, 1, to, :] = (s0 * lr + c0 * li) + (s1 * rr + c1 * ri)

    def consume(t, begin, end):
        j = chunk_of(t)
        for d in (2, 1, 3):
            window_copy(t, d).wait_recv()
        make_parents(j)

        def fine_in(s, carry, e, weights):
            slot = pl.multiple_of(s * SUB, SUB)
            fine_two(j * CHUNK - 2 * RIM + slot, slot, e, weights)
            return carry

        def coarse_in(s, carry, e, picks):
            slot = pl.multiple_of(s * SUB, SUB)
            coarse_two(slot, slot, e, picks)
            return carry

        def rows_out(s, carry):
            slot = pl.multiple_of(s * SUB, SUB)
            finish(pl.multiple_of(j * CHUNK - RIM + slot, SUB), slot, j, slot)
            return carry

        for e in range(2):
            lax.fori_loop(
                begin, end + 1, functools.partial(fine_in, e=e, weights=weights_two(e)), 0
            )
            lax.fori_loop(
                begin, end, functools.partial(coarse_in, e=e, picks=picks_of(step2.at[e])), 0
            )
        products(end * SUB)
        lax.fori_loop(begin, end, rows_out, 0)

    def step(t, carry):
        j = chunk_of(t)

        @pl.when(t + LEAD - 1 < CHUNKS)
        def _():
            send(t + LEAD - 1)

        @pl.when(t + LEAD < CHUNKS)
        def _():
            @pl.when(t + LEAD == CHUNKS - 1 - FIRST)
            def _():
                for c in zc:
                    c.wait_recv()

                @pl.when(rng == 0)
                def _():
                    child[:, 0:RIM, :] = jnp.zeros((2, RIM, BEAM), F32)

                @pl.when(rng == 3)
                def _():
                    child[:, RIM + ROWS :, :] = jnp.zeros((2, RIM, BEAM), F32)

            produce(t + LEAD)
            edge_copy(t + LEAD).start()

        consume(t, jnp.where(jnp.logical_or(t == 0, j == 0), 2, 0), CHUNK // SUB)

        @pl.when(j == 0)
        def _():
            zp[0].start()

        @pl.when(j == CHUNKS - 1)
        def _():
            zp[1].start()

        return carry

    lax.fori_loop(0, CHUNKS - 1, step, 0)

    for c in zp:
        c.wait_recv()

    @pl.when(rng == 0)
    def _():
        parent[:, TOP - RIM : TOP, :] = jnp.zeros((4, RIM, BEAM), F32)

    @pl.when(rng == 3)
    def _():
        parent[:, TOP + ROWS : TOP + ROWS + RIM, :] = jnp.zeros((4, RIM, BEAM), F32)

    ends = ((0, 0, RIM), (ROWS - RIM, CHUNKS, 0))
    for n, (first, j, rho) in enumerate(ends):
        for e in range(2):
            for half in range(2):
                fine_two(first - RIM + half * SUB, half * SUB, e, weights_two(e))
            coarse_two(n * SUB, 0, e, picks_of(step2.at[e]))
    products(len(ends) * SUB)
    for n, (first, j, rho) in enumerate(ends):
        finish(first, n * SUB, j, rho)

    consume(CHUNKS - 1, 0, CHUNK // SUB + 2)

    for c in zc + zp:
        c.wait_send()

    def drain(t, carry):
        edge_copy(t).wait_send()
        for d in (2, 1, 3):
            window_copy(t, d).wait_send()
        return carry

    lax.fori_loop(0, CHUNKS, drain, 0)


def body(*args):
    dma = pltpu.SemaphoreType.DMA
    args = [pltpu.with_memory_space_constraint(a, pltpu.HBM) for a in args]
    return pl.pallas_call(
        kernel,
        out_shape=jax.ShapeDtypeStruct((1, 2, ROWS, BEAM), F32),
        in_specs=[pl.BlockSpec(memory_space=pl.ANY)] * 13,
        out_specs=pl.BlockSpec(memory_space=pltpu.VMEM),
        scratch_shapes=[pltpu.VMEM(a.shape, a.dtype) for a in args[1:]]
        + [
            pltpu.VMEM((2, ROWS + 2 * RIM, BEAM), F32),
            pltpu.VMEM((2, CHUNK, BEAM), F32),
            pltpu.VMEM((2, BEAM + 16, ROWS), F32),
            pltpu.VMEM((4, 2, WIN, ROWS), F32),
            pltpu.VMEM((8, NEAR, BEAM), F32),
            pltpu.VMEM((4, TOP + ROWS + 32, BEAM), F32),
            pltpu.VMEM((4, NEAR, 2 * BEAM), BF16),
            pltpu.VMEM((FINE, 8, BEAM), F32),
            pltpu.VMEM((2, FINE, 8, BEAM), F32),
            pltpu.VMEM((8, BEAM), jnp.int32),
            pltpu.VMEM((2, 8, BEAM), jnp.int32),
            pltpu.VMEM((4, NEAR + SUB, BEAM), F32),
            pltpu.VMEM((2, 3 * WIN, BEAM), BF16),
            pltpu.VMEM((2, 2 * BEAM, BEAM), BF16),
            pltpu.VMEM((2, BEAM, BEAM), BF16),
            pltpu.VMEM((4, NEAR, BEAM), F32),
            pltpu.VMEM((4, NEAR, BEAM), F32),
            pltpu.VMEM((4, FAR, BEAM), F32),
            pltpu.VMEM((4, FAR, BEAM), F32),
            pltpu.VMEM((24, BEAM), F32),
            pltpu.VMEM((24, BEAM), F32),
            dma((3,)),
            dma((12,)),
            pltpu.SemaphoreType.REGULAR,
            pltpu.SemaphoreType.REGULAR,
            dma((2,)),
            dma((2,)),
            dma((2,)),
            dma((2,)),
            dma((CHUNKS,)),
            dma((CHUNKS,)),
            dma((3, CHUNKS)),
            dma((3, CHUNKS)),
        ],
        compiler_params=pltpu.CompilerParams(
            collective_id=0, has_side_effects=True, vmem_limit_bytes=36 * 2**20
        ),
        name="merge",
    )(*args)


def solution(mesh):
    return jax.shard_map(
        body,
        mesh=mesh,
        in_specs=(P("aper", None, "rng", "beam"),) + (P(),) * 12,
        out_specs=P("aper", None, "rng", "beam"),
        check_vma=False,
    )
```
